32 devices in a mesh: ta: 4 (over z), gz: 2 (over x), xy: 4 (over y, core).
Axes of the slice: x: 2, y: 2, z: 4, core: 2. Of those that a mesh axis runs over, the one named last changes fastest.
Arguments:
- links: float32 [4, 2, 4, 4, 9, 4608], P('ta', 'gz', 'xy'), may hold values from -1 to 3
- eigvecs: float32 [4, 2, 4, 4, 48, 128], P('ta', 'gz', 'xy'), may hold values from -1 to 1
- eig_real: float32 [64], replicated, may hold values from 0.8 to 2.5
- eig_imag: float32 [64], replicated, may hold values from -0.5 to 0.5
- rhs: float32 [4, 2, 4, 4, 48, 128], P('ta', 'gz', 'xy'), may hold values from -3000 to 3000
Outputs:
- solution: float32 [4, 2, 4, 4, 48, 128], P('ta', 'gz', 'xy')
- residual: float32 [4, 2, 4, 4, 48, 128], P('ta', 'gz', 'xy')
The draws below stay inside these ranges and needn't reach their ends.
All inputs are finite; a program needn't handle non-finite values.
Results may differ from the reference program's by a relative error of at most 0.0003.
Values sent between devices are 32-bit elements; how exact they have to be, the bound alone decides.
A program may use at most 64 MiB of HBM per device.

```python
import jax
import jax.numpy as jnp
from jax import lax

DOF = 48
NEV = 64
NRHS = 64
SWEEPS = 4
NT = 4
NZ = 2
NX = 4
NY = 4


def eigen_fields(key):
    shape = (NT, NZ, NX, NY, DOF, 2 * NEV)
    values = jnp.clip(jax.random.normal(key, shape, jnp.float32), -4.0, 4.0)
    return values / jnp.sqrt(jnp.float32(NT * NZ * NX * NY * DOF * 2))


def draw_eigvecs(key, part):
    return eigen_fields(jax.random.fold_in(key, 7))


def draw_rhs(key, part):
    vectors = eigen_fields(jax.random.fold_in(key, 7))
    keys = jax.random.split(jax.random.fold_in(key, 13), 4)
    spread = jnp.sqrt(jnp.float32(NT * NZ * NX * NY * DOF * 2) / jnp.float32(2 * NEV))
    weights = jnp.clip(jax.random.normal(keys[0], (2 * NEV, NRHS), jnp.float32), -4.0, 4.0) * spread
    w_re = weights[:NEV]
    w_im = weights[NEV:]
    block = jnp.concatenate([jnp.concatenate([w_re, w_im], 1), jnp.concatenate([-w_im, w_re], 1)], 0)
    along = jnp.einsum('tzxydk,kc->tzxydc', vectors, block, precision=lax.Precision.HIGHEST)
    site_scale = jnp.exp(jax.random.uniform(keys[1], (NT, NZ, NX, NY, 1, 1), jnp.float32, 0.0, 2.3026))
    column = jnp.exp(jax.random.uniform(keys[2], (NRHS,), jnp.float32, 0.0, 2.3026))
    column = jnp.concatenate([column, column])
    ramp_t = 3.0 ** (jnp.arange(NT, dtype=jnp.float32) / max(NT - 1, 1))
    ramp_z = 3.0 ** (jnp.arange(NZ, dtype=jnp.float32) / max(NZ - 1, 1))
    ramp_x = 3.0 ** (jnp.arange(NX, dtype=jnp.float32) / max(NX - 1, 1))
    ramp = ramp_t[:, None, None] * ramp_z[None, :, None] * ramp_x[None, None, :]
    ramp = ramp[:, :, :, None, None, None]
    shape = (NT, NZ, NX, NY, DOF, 2 * NRHS)
    noise = jnp.clip(jax.random.normal(keys[3], shape, jnp.float32), -4.0, 4.0)
    return along + noise * site_scale * column * ramp / 30.0


def draw_links(key, part):
    keys = jax.random.split(jax.random.fold_in(key, 21), 2)
    shape = (NT, NZ, NX, NY, 9, DOF, 2 * DOF)
    noise = jnp.clip(jax.random.normal(keys[0], shape, jnp.float32), -4.0, 4.0)
    own = (jnp.arange(9) == 0).astype(jnp.float32)
    factor = 0.01 + 0.01 * own
    noise = noise * factor[:, None, None]
    mass = jax.random.uniform(keys[1], (NT, NZ, NX, NY, 1, 1, 1), jnp.float32, 1.0, 2.5)
    identity = jnp.eye(DOF, 2 * DOF, dtype=jnp.float32)
    full = noise + mass * identity[None, :, :] * own[:, None, None]
    return full.reshape(NT, NZ, NX, NY, 9, 2 * DOF * DOF)


def setup_inputs(seed: int = 0) -> dict:
    streams_of = jax.random.split(jax.random.key(seed), 6)
    links = draw_links(jax.random.fold_in(streams_of[5], 71), 0)
    eigvecs = draw_eigvecs(jax.random.fold_in(streams_of[5], 71), 0)
    eig_real = jnp.clip(jax.random.uniform(streams_of[2], (NEV,), jnp.float32, 0.8, 2.5), 0.8, 2.5)
    eig_imag = jnp.clip(jax.random.uniform(streams_of[3], (NEV,), jnp.float32, -0.5, 0.5), -0.5, 0.5)
    rhs = draw_rhs(jax.random.fold_in(streams_of[5], 71), 0)
    return {"links": links, "eigvecs": eigvecs, "eig_real": eig_real, "eig_imag": eig_imag, "rhs": rhs}


HIGH = lax.Precision.HIGHEST


def link_apply(matrix, field):
    half = field.shape[-1] // 2
    real = jnp.einsum('tzxyoi,tzxyic->tzxyoc', matrix[..., :DOF], field, precision=HIGH)
    imag = jnp.einsum('tzxyoi,tzxyic->tzxyoc', matrix[..., DOF:], field, precision=HIGH)
    return jnp.concatenate([real[..., :half] - imag[..., half:], real[..., half:] + imag[..., :half]], -1)


def operate(links, field):
    total = link_apply(links[:, :, :, :, 0], field)
    for axis in range(4):
        total = total - link_apply(links[:, :, :, :, 1 + axis], jnp.roll(field, -1, axis))
        total = total - link_apply(links[:, :, :, :, 5 + axis], jnp.roll(field, 1, axis))
    return total


def complex_scale(alpha_re, alpha_im, field):
    half = field.shape[-1] // 2
    f_re = field[..., :half]
    f_im = field[..., half:]
    return jnp.concatenate([alpha_re * f_re - alpha_im * f_im, alpha_re * f_im + alpha_im * f_re], -1)


def reference(links, eigvecs, eig_real, eig_imag, rhs):
    links = links.reshape(NT, NZ, NX, NY, 9, DOF, 2 * DOF)
    rows = eigvecs.reshape(-1, 2 * NEV)
    cross = jnp.dot(rows.T, rhs.reshape(-1, 2 * NRHS), precision=HIGH, preferred_element_type=jnp.float32)
    proj_re = cross[:NEV, :NRHS] + cross[NEV:, NRHS:]
    proj_im = cross[:NEV, NRHS:] - cross[NEV:, :NRHS]
    denom = (eig_real * eig_real + eig_imag * eig_imag)[:, None]
    coef_re = (proj_re * eig_real[:, None] + proj_im * eig_imag[:, None]) / denom
    coef_im = (proj_im * eig_real[:, None] - proj_re * eig_imag[:, None]) / denom
    block = jnp.concatenate([jnp.concatenate([coef_re, coef_im], 1), jnp.concatenate([-coef_im, coef_re], 1)], 0)
    solution = jnp.dot(rows, block, precision=HIGH, preferred_element_type=jnp.float32).reshape(rhs.shape)
    residual = rhs - operate(links, solution)
    for sweep in range(SWEEPS):
        image = operate(links, residual)
        swapped = jnp.concatenate([residual[..., NRHS:], residual[..., :NRHS]], -1)
        first = jnp.sum(image * residual, axis=(0, 1, 2, 3, 4))
        second = jnp.sum(image * swapped, axis=(0, 1, 2, 3, 4))
        power = jnp.sum(image * image, axis=(0, 1, 2, 3, 4))
        num_re = first[:NRHS] + first[NRHS:]
        num_im = second[:NRHS] - second[NRHS:]
        den = power[:NRHS] + power[NRHS:]
        alpha_re = num_re / den
        alpha_im = num_im / den
        solution = solution + complex_scale(alpha_re, alpha_im, residual)
        residual = residual - complex_scale(alpha_re, alpha_im, image)
    return solution, residual
```

```python
import functools

import jax
import jax.numpy as jnp
from jax import lax
from jax.experimental import pallas as pl
from jax.experimental.pallas import tpu as pltpu
from jax.sharding import PartitionSpec as P

SWEEPS = 4
DIRECT = 32
MESH = pl.DeviceIdType.MESH
F32, BF16 = jnp.float32, jnp.bfloat16


def split(x):
    first = x.astype(BF16)
    return first, (x - first.astype(F32)).astype(BF16)


def pair(x):
    return jnp.concatenate(split(x), 1)


def pad_to(n, m):
    return -(-n // m) * m


def kernel(
    sizes, dims, links_hbm, v_hbm, er_hbm, ei_hbm, rhs_hbm, sol_ref, res_ref,
    links, v_ref, rhs_ref, er_ref, ei_ref, flat, mats, acc, pcs, fields, halos, vw, start_ref,
    g_ref, cpart, rs_buf, ct_buf, ag_buf, ec, st_buf, sp_buf, sd_buf,
    in_sem, halo_send, halo_recv, rs_send, rs_recv, ct_send, ct_recv, ag_send, ag_recv,
    st_send, st_recv, sp_send, sp_recv, sd_send, sd_recv,
):
    nt, nz, nx = sizes
    ny, dof, lanes = dims
    half = lanes // 2
    plane = nz * nx
    it, iz, ix = lax.axis_index("ta"), lax.axis_index("gz"), lax.axis_index("xy")
    me = iz * nx + ix
    part = half // plane

    loads = []
    for i, (src, dst) in enumerate(
        ((v_hbm, v_ref), (rhs_hbm, rhs_ref), (links_hbm, links), (er_hbm, er_ref), (ei_hbm, ei_ref))
    ):
        c = pltpu.make_async_copy(src, dst, in_sem.at[i])
        c.start()
        loads.append(c)

    def plane_peer(k):
        p = lax.rem(me + k, plane)
        return p, {"ta": it, "gz": lax.div(p, nx), "xy": lax.rem(p, nx)}

    def time_peer(k):
        p = lax.rem(it + k, nt)
        return p, {"ta": p, "gz": iz, "xy": ix}

    everyone = nt * plane
    rank = it * plane + me

    def any_peer(k):
        p = lax.rem(rank + k, everyone)
        r = lax.rem(p, plane)
        return p, {"ta": lax.div(p, plane), "gz": lax.div(r, nx), "xy": lax.rem(r, nx)}

    direct = everyone <= DIRECT
    greeted = [plane_peer(k)[1] for k in range(1, plane)]
    greeted += [time_peer(k)[1] for k in range(1, nt)]
    barrier = pltpu.get_barrier_semaphore()
    for target in greeted:
        pl.semaphore_signal(barrier, inc=1, device_id=target, device_id_type=MESH)

    def neighbours(axis, index, n):
        base = {"ta": it, "gz": iz, "xy": ix}
        up, down = dict(base), dict(base)
        up[axis] = lax.rem(index + 1, n)
        down[axis] = lax.rem(index + n - 1, n)
        return up, down

    outgoing, groups, slot = [], {}, 0
    for axis, index, n, d in (("ta", it, nt, 1), ("xy", ix, nx, 3), ("gz", iz, nz, 2)):
        up, down = neighbours(axis, index, n)
        if n == 2:
            outgoing.append((axis, slot, up))
            groups[axis] = [(slot, (d, d + 4))]
            slot += 1
        else:
            turn = jnp.where(index == n - 1, 1, 0)
            for t in (turn, 1 - turn):
                target = dict(up)
                target[axis] = lax.rem(index + n - 1 + 2 * t, n)
                outgoing.append((axis, slot + t, target))
            groups[axis] = [(slot, (d,)), (slot + 1, (d + 4,))]
            slot += 2
    far, near = groups["ta"], groups["xy"] + groups["gz"]
    sends = []

    def send_chunk(rnd, src, y, axes=("ta", "xy", "gz")):
        for axis, s, target in outgoing:
            if axis not in axes:
                continue
            c = pltpu.make_async_remote_copy(
                src_ref=src.at[y], dst_ref=halos.at[rnd, s, y],
                send_sem=halo_send.at[rnd, s, y], recv_sem=halo_recv.at[rnd, s, y],
                device_id=target, device_id_type=MESH,
            )
            c.start()
            sends.append(c)

    def arrived(rnd, s, y):
        pltpu.make_async_remote_copy(
            src_ref=v_ref.at[y], dst_ref=halos.at[rnd, s, y],
            send_sem=halo_send.at[rnd, s, y], recv_sem=halo_recv.at[rnd, s, y],
            device_id=outgoing[0][2], device_id_type=MESH,
        ).wait_recv()

    def share(buf, mine, n, peer, send, recv):
        out = []
        for k in range(1, n):
            c = pltpu.make_async_remote_copy(
                src_ref=buf.at[mine], dst_ref=buf.at[mine],
                send_sem=send.at[k], recv_sem=recv.at[k],
                device_id=peer(k)[1], device_id_type=MESH,
            )
            c.start()
            out.append(c)
        sends.extend(out)
        return out

    def recv_all(copies):
        for c in copies:
            c.wait_recv()

    def add_slots(buf, n):
        parts = [buf[p] for p in range(n)]
        while len(parts) > 1:
            odd = parts[len(parts) // 2 * 2 :]
            parts = [a + b for a, b in zip(parts[::2], parts[1::2])] + odd
        return parts[0]

    lane = lax.broadcasted_iota(jnp.int32, (1, lanes), 1)
    low = lane < half
    jsign = jnp.where(low, -1.0, 1.0).astype(F32)

    def swap(x):
        return pltpu.roll(x, half, 1)

    def real(c):
        return jnp.where(low, c, swap(c))

    def imag(c):
        return jnp.where(low, swap(c), c)

    def factor(c):
        return real(c), imag(c) * jsign

    def times(f, x):
        return f[0] * x + f[1] * swap(x)

    def mul(a, b):
        return times(factor(a), b)

    def conj(a):
        return -jsign * a

    one = jnp.where(low, 1.0, 0.0).astype(F32)

    loads[0].wait()
    loads[1].wait()
    rows = pair(v_ref[...].reshape(ny * dof, lanes))
    cross = lax.dot_general(
        rows, pair(rhs_ref[...].reshape(ny * dof, lanes)), (((0,), (0,)), ((), ())),
        preferred_element_type=F32,
    )
    cross = cross[:lanes, :lanes] + (cross[:lanes, lanes:] + cross[lanes:, :lanes])
    corr = cross[:half] - jsign * swap(cross[half:])
    for p in range(plane):
        cpart[p] = corr[p * part : (p + 1) * part]
    pl.semaphore_wait(barrier, len(greeted))
    rs_copies = []
    for k in range(1, plane):
        p, target = plane_peer(k)
        c = pltpu.make_async_remote_copy(
            src_ref=cpart.at[p], dst_ref=rs_buf.at[me],
            send_sem=rs_send.at[k], recv_sem=rs_recv.at[k],
            device_id=target, device_id_type=MESH,
        )
        c.start()
        rs_copies.append(c)
    rs_buf[me] = cpart[me]
    sends += rs_copies
    for y in range(ny):
        send_chunk(0, v_ref, y, ("xy", "gz"))

    loads[3].wait()
    loads[4].wait()
    theta = half / jnp.sum(er_ref[...], axis=1, keepdims=True)
    eye = lax.broadcasted_iota(jnp.int32, (half, half), 0) == lax.broadcasted_iota(
        jnp.int32, (half, half), 1
    )
    er = jnp.sum(jnp.where(eye, er_ref[...], 0.0), axis=1, keepdims=True)
    ei = jnp.sum(jnp.where(eye, ei_ref[...], 0.0), axis=1, keepdims=True)
    scale = 1.0 / (er * er + ei * ei)
    ec[0] = er * scale + jnp.zeros((half, lanes), F32)
    ec[1] = -jsign * (ei * scale)

    loads[2].wait()
    two = 2 * dof
    valid = lane < two

    def pick(ds, b, j):
        at = j * two
        base, off = (at // 128) * 128, at % 128
        start = pl.multiple_of(b * (4 * two), 128) + base
        width = 128 if off + two <= 128 else 256
        x = [links[d, :, pl.ds(start, width)] for d in ds]
        x = jnp.concatenate(x, 0) if len(x) > 1 else x[0]
        if off:
            x = pltpu.roll(x, width - off, 1)
        return jnp.where(valid, x[:, :128], 0.0)

    def relayout(b, carry):
        for ds in ((0, 1), (2, 3), (4, 5), (6, 7), (8,)):
            for j in range(4):
                row = ds[0] * ny * dof + 4 * b + j
                flat[pl.ds(row, len(ds) * ny, stride=dof), :] = pick(ds, b, j)
        return carry

    lax.fori_loop(0, dof // 4, relayout, 0)

    def direction(y, d):
        return flat[pl.ds((d * ny + y) * dof, dof), :]

    local_group = [(0,), (4,), (8,)]
    near_group = [ds for _, ds in near]
    far_group = [ds for _, ds in far]
    widths = [pad_to(len(g) * dof, 128) for g in (local_group, near_group, far_group)]
    bases = [0, widths[0], widths[0] + widths[1]]
    first_half = lane < dof
    diag = jnp.where(
        lax.broadcasted_iota(jnp.int32, (dof, lanes), 0)
        == lax.broadcasted_iota(jnp.int32, (dof, lanes), 1), 1.0, 0.0,
    )

    def place(parts, width):
        tiles = [jnp.zeros((dof, 128), F32)] * (width // 128)
        for m, p in enumerate(parts):
            t, w = divmod(dof * m, 128)
            r = pltpu.roll(p, w, 1) if w else p
            if w + dof <= 128:
                tiles[t] = tiles[t] + r
            else:
                tiles[t] = tiles[t] + jnp.where(lane >= w, r, 0.0)
                tiles[t + 1] = tiles[t + 1] + jnp.where(lane < w, r, 0.0)
        return jnp.concatenate(tiles, 1)

    def build(y):
        for g, group in enumerate((local_group, near_group, far_group)):
            res, ims = [], []
            for ds in group:
                x = direction(y, ds[0])
                for d in ds[1:]:
                    x = x + direction(y, d)
                x = x * theta
                if not ds[0]:
                    x = diag - x
                res.append(jnp.where(first_half, x, 0.0))
                ims.append(jnp.where(first_half, pltpu.roll(x, 128 - dof, 1), 0.0))
            for h, parts in enumerate((res, ims)):
                for i, piece in enumerate(split(place(parts, widths[g]))):
                    row = (2 * i + h) * dof
                    mats[y, row : row + dof, bases[g] : bases[g] + widths[g]] = piece

    def product(y, g, blocks):
        width = widths[g]
        rest = width - len(blocks) * dof
        if rest:
            blocks = blocks + [jnp.zeros((rest, 2 * lanes), BF16)]
        out = jnp.dot(
            mats[y, :, bases[g] : bases[g] + width], jnp.concatenate(blocks, 0),
            preferred_element_type=F32,
        )
        return out[:two, :lanes] + (out[:two, lanes:] + out[two:, :lanes])

    def begin():
        for y in range(ny):
            acc[y] = product(y, 0, [pcs[y], pcs[(y + 1) % ny], pcs[(y - 1) % ny]])

    def halo_blocks(rnd, y, group):
        blocks = []
        for s, _ in group:
            arrived(rnd, s, y)
            blocks.append(pair(halos[rnd, s, y]))
        return blocks

    def middle(rnd, y):
        acc[y] += product(y, 1, halo_blocks(rnd, y, near))

    def finish(rnd, y):
        t = acc[y] + product(y, 2, halo_blocks(rnd, y, far))
        return t[:dof] + jsign * swap(t[dof:])

    recv_all(rs_copies)
    ct_buf[it] = add_slots(rs_buf, plane)
    ct_copies = share(ct_buf, it, nt, time_peer, ct_send, ct_recv)
    for y in range(ny):
        send_chunk(0, v_ref, y, ("ta",))

    for y in range(ny):
        build(y)
    for y in range(ny):
        pcs[y] = pair(v_ref[y])
    begin()

    recv_all(ct_copies)
    total = add_slots(ct_buf, nt)
    mine = pl.ds(me * part, part)
    ag_buf[me] = total * ec[0, mine] + swap(total) * ec[1, mine]
    ag_copies = share(ag_buf, me, plane, plane_peer, ag_send, ag_recv)

    for y in range(ny):
        middle(0, y)
    inverse = 1.0 / theta
    for y in range(ny):
        v = v_ref[y]
        w = (v - finish(0, y)) * inverse
        for i, piece in enumerate(split(w) + split(v)):
            vw[y, i * dof : (i + 1) * dof] = piece

    recv_all(ag_copies)
    coef = jnp.concatenate([ag_buf[p] for p in range(plane)], 0)
    block = pair(jnp.concatenate([coef, jsign * swap(coef)], 0))

    def expand(y, i):
        out = jnp.dot(vw[y, i * dof : (i + 2) * dof], block, preferred_element_type=F32)
        return out[:dof, :lanes] + (out[:dof, lanes:] + out[dof:, :lanes])

    for y in range(ny):
        r = rhs_ref[y] - expand(y, 0)
        fields[0, y] = r
        send_chunk(1, fields.at[0], y)
        pcs[y] = pair(r)
    for y in range(ny):
        start_ref[y] = expand(y, 2)

    def fold(x):
        return jnp.sum(x.reshape(dof // 8, 8, lanes), axis=0)

    def partials(x0, x1, x2):
        u0, u1 = x0 - x1, x1 - x2
        s0, t0 = swap(x0), swap(u0)
        return [
            fold(p)
            for p in (u0 * x0, u0 * s0, u1 * x0, u1 * s0, u1 * u0, u1 * t0, u0 * u0, u1 * u1)
        ]

    def add(a, b):
        return b if a is None else [p + q for p, q in zip(a, b)]

    def gram(sums):
        s = [jnp.sum(p, axis=0, keepdims=True) for p in sums]
        out = [
            jnp.where(low, s[i] + swap(s[i]), swap(s[i + 1]) - s[i + 1]) for i in (0, 2, 4)
        ]
        out.append(jnp.where(low, s[6] + swap(s[6]), s[7] + swap(s[7])))
        row = lax.broadcasted_iota(jnp.int32, (4, lanes), 0)
        x = out[3]
        for i in (2, 1, 0):
            x = jnp.where(row == i, out[i], x)
        return x

    def steps(total):
        a, b, c, d = (total[i : i + 1] for i in range(4))
        b0 = a / real(d)
        e = mul(conj(b0), c)
        num = mul(conj(b0), b) - mul(real(mul(conj(b0), b0)) * one, c)
        near_one = one - b0
        size0 = real(mul(conj(near_one), near_one))
        size1 = real(mul(conj(b0), b0))
        den = size0 * real(d) + size1 * imag(d) + 2.0 * real(mul(near_one, e))
        b1 = num / den
        both = mul(b0, b1)
        mixed = b0 + b1 - both
        poly = [factor(x) for x in (one - mixed, mixed - both, both)]
        gain = [factor(theta * x) for x in (mixed, both)]
        return poly, gain

    def combine(poly, xs):
        out = times(poly[0], xs[0])
        for p, x in zip(poly[1:], xs[1:]):
            out = out + times(p, x)
        return out

    def step(rnd, y):
        out = finish(rnd, y)
        fields[rnd, y] = out
        if rnd < SWEEPS:
            send_chunk(rnd + 1, fields.at[rnd], y)
            pcs[y] = pair(out)

    LEAD = 2
    poly = gain = None
    sums = None
    for rnd in range(1, SWEEPS + 1):
        begin()
        if rnd == 3:
            for y in range(ny):
                sums = add(sums, partials(fields[0, y], fields[1, y], fields[2, y]))
            st_buf[0, it] = gram(sums)
            early = share(st_buf.at[0], it, nt, time_peer, st_send.at[0], st_recv.at[0])
        if rnd == 4:
            recv_all(early)
            sp_buf[0, me] = add_slots(st_buf.at[0], nt)
            early = share(sp_buf.at[0], me, plane, plane_peer, sp_send.at[0], sp_recv.at[0])
        for y in range(ny + LEAD):
            if y < ny:
                middle(rnd, y)
            if y >= LEAD:
                step(rnd, y - LEAD)
    recv_all(early)
    poly, gain = steps(add_slots(sp_buf.at[0], plane))
    sums = None
    for y in range(ny):
        f = [fields[i, y] for i in range(SWEEPS + 1)]
        g = [combine(poly, f[i : i + 3]) for i in range(3)]
        for i in range(3):
            g_ref[i, y] = g[i]
        start_ref[y] = start_ref[y] + combine(gain, f[:2])
        sums = add(sums, partials(*g))
    if direct:
        sd_buf[rank] = gram(sums)
        last = share(sd_buf, rank, everyone, any_peer, sd_send, sd_recv)
        recv_all(last)
        total = add_slots(sd_buf, everyone)
    else:
        st_buf[1, it] = gram(sums)
        last = share(st_buf.at[1], it, nt, time_peer, st_send.at[1], st_recv.at[1])
        recv_all(last)
        sp_buf[1, me] = add_slots(st_buf.at[1], nt)
        last = share(sp_buf.at[1], me, plane, plane_peer, sp_send.at[1], sp_recv.at[1])
        recv_all(last)
        total = add_slots(sp_buf.at[1], plane)
    poly, gain = steps(total)
    for y in range(ny):
        g = [g_ref[i, y] for i in range(3)]
        sol_ref[y] = start_ref[y] + combine(gain, g[:2])
        res_ref[y] = combine(poly, g)
    for c in sends:
        c.wait_send()


def hand_over(a_ref, b_ref, sol_ref, res_ref):
    sol_ref[...] = a_ref[...]
    res_ref[...] = b_ref[...]


def local(sizes, links, eigvecs, eig_real, eig_imag, rhs):
    nt, nz, nx = sizes
    plane = nz * nx
    ny, dof, lanes = rhs.shape[3:]
    half = lanes // 2
    field = (ny, dof, lanes)
    ndir = links.shape[4]
    slots = sum(1 if n == 2 else 2 for n in sizes)
    far = 1 if nt == 2 else 2
    part = half // plane
    rounds = SWEEPS + 1
    everyone = nt * plane
    direct = everyone if everyone <= DIRECT else 1
    width = sum(pad_to(n * dof, 128) for n in (3, slots - far, far))
    vmem, dma = pltpu.VMEM, pltpu.SemaphoreType.DMA
    spec = pl.BlockSpec(memory_space=pltpu.VMEM)
    sol, res = pl.pallas_call(
        functools.partial(kernel, sizes, field),
        out_shape=[jax.ShapeDtypeStruct(field, F32)] * 2,
        in_specs=[pl.BlockSpec(memory_space=pl.ANY)] * 5,
        out_specs=[spec] * 2,
        scratch_shapes=[
            vmem((ndir, ny, links.shape[5]), F32),
            vmem(field, F32),
            vmem(field, F32),
            vmem((1, half), F32),
            vmem((1, half), F32),
            vmem((ndir * ny * dof, 128), F32),
            vmem((ny, 4 * dof, width), BF16),
            vmem((ny, 2 * dof, lanes), F32),
            vmem((ny, dof, 2 * lanes), BF16),
            vmem((rounds,) + field, F32),
            vmem((rounds, slots) + field, F32),
            vmem((ny, 4 * dof, lanes), BF16),
            vmem(field, F32),
            vmem((3,) + field, F32),
            vmem((plane, part, lanes), F32),
            vmem((plane, part, lanes), F32),
            vmem((nt, part, lanes), F32),
            vmem((plane, part, lanes), F32),
            vmem((2, half, lanes), F32),
            vmem((2, nt, 4, lanes), F32),
            vmem((2, plane, 4, lanes), F32),
            vmem((direct, 4, lanes), F32),
            dma((5,)),
            dma((rounds, slots, ny)),
            dma((rounds, slots, ny)),
            dma((plane,)),
            dma((plane,)),
            dma((nt,)),
            dma((nt,)),
            dma((plane,)),
            dma((plane,)),
            dma((2, nt)),
            dma((2, nt)),
            dma((2, plane)),
            dma((2, plane)),
            dma((direct,)),
            dma((direct,)),
        ],
        compiler_params=pltpu.CompilerParams(collective_id=0, has_side_effects=True),
    )(
        links.reshape(links.shape[3:]).transpose(1, 0, 2),
        eigvecs.reshape(field),
        eig_real.reshape(1, -1),
        eig_imag.reshape(1, -1),
        rhs.reshape(field),
    )
    sol, res = pl.pallas_call(
        hand_over,
        out_shape=[jax.ShapeDtypeStruct(field, F32)] * 2,
        in_specs=[spec] * 2,
        out_specs=[spec] * 2,
    )(sol, res)
    return (sol.reshape(rhs.shape), res.reshape(rhs.shape))


def solution(mesh):
    whole = P("ta", "gz", "xy", None, None, None)
    sizes = tuple(mesh.shape[a] for a in ("ta", "gz", "xy"))
    return jax.shard_map(
        functools.partial(local, sizes),
        mesh=mesh,
        in_specs=(whole, whole, P(), P(), whole),
        out_specs=(whole, whole),
        check_vma=False,
    )
```

```python
import functools

import jax
import jax.numpy as jnp
from jax import lax
from jax.experimental import pallas as pl
from jax.experimental.pallas import tpu as pltpu
from jax.sharding import PartitionSpec as P

SWEEPS = 4
LEAD = 0
AHEAD = 0
DIRECT = 32
MESH = pl.DeviceIdType.MESH
F32, BF16 = jnp.float32, jnp.bfloat16


def split(x):
    first = x.astype(BF16)
    return first, (x - first.astype(F32)).astype(BF16)


def pair(x):
    return jnp.concatenate(split(x), 1)


def pad_to(n, m):
    return -(-n // m) * m


def kernel(
    sizes, dims, links_hbm, v_hbm, er_hbm, ei_hbm, rhs_hbm, sol_ref, res_ref,
    links, v_ref, rhs_ref, er_ref, ei_ref, flat, mats, acc, pcs, fields, halos, vw, image_ref, start_ref,
    g_ref, cpart, rs_buf, ct_buf, ag_buf, ec, st_buf, sp_buf, sd_buf,
    in_sem, halo_send, halo_recv, rs_send, rs_recv, ct_send, ct_recv, ag_send, ag_recv,
    st_send, st_recv, sp_send, sp_recv, sd_send, sd_recv,
):
    nt, nz, nx = sizes
    ny, dof, lanes = dims
    half = lanes // 2
    plane = nz * nx
    it, iz, ix = lax.axis_index("ta"), lax.axis_index("gz"), lax.axis_index("xy")
    me = iz * nx + ix
    part = half // plane

    loads = []
    for i, (src, dst) in enumerate(
        ((v_hbm, v_ref), (rhs_hbm, rhs_ref), (links_hbm, links), (er_hbm, er_ref), (ei_hbm, ei_ref))
    ):
        c = pltpu.make_async_copy(src, dst, in_sem.at[i])
        c.start()
        loads.append(c)

    def ranked(*ns):
        steps = [()]
        for n in ns:
            steps = [o + (d,) for o in steps for d in range(n)]
        steps.sort(key=lambda o: -sum(min(d, n - d) for d, n in zip(o, ns)))
        return steps[-1:] + steps[:-1]

    plane_steps, all_steps = ranked(nz, nx), ranked(nt, nz, nx)

    def plane_peer(k):
        dz, dx = plane_steps[k]
        z, x = lax.rem(iz + dz, nz), lax.rem(ix + dx, nx)
        return z * nx + x, {"ta": it, "gz": z, "xy": x}

    def time_peer(k):
        p = lax.rem(it + k, nt)
        return p, {"ta": p, "gz": iz, "xy": ix}

    everyone = nt * plane
    rank = it * plane + me

    def any_peer(k):
        dt, dz, dx = all_steps[k]
        t, z, x = lax.rem(it + dt, nt), lax.rem(iz + dz, nz), lax.rem(ix + dx, nx)
        return t * plane + z * nx + x, {"ta": t, "gz": z, "xy": x}

    direct = everyone <= DIRECT
    greeted = [plane_peer(k)[1] for k in range(1, plane)]
    greeted += [time_peer(k)[1] for k in range(1, nt)]
    barrier = pltpu.get_barrier_semaphore()
    for target in greeted:
        pl.semaphore_signal(barrier, inc=1, device_id=target, device_id_type=MESH)

    def neighbours(axis, index, n):
        base = {"ta": it, "gz": iz, "xy": ix}
        up, down = dict(base), dict(base)
        up[axis] = lax.rem(index + 1, n)
        down[axis] = lax.rem(index + n - 1, n)
        return up, down

    outgoing, groups, slot = [], {}, 0
    for axis, index, n, d in (("ta", it, nt, 1), ("xy", ix, nx, 3), ("gz", iz, nz, 2)):
        up, down = neighbours(axis, index, n)
        if n == 2:
            outgoing.append((axis, slot, up))
            groups[axis] = [(slot, (d, d + 4))]
            slot += 1
        else:
            turn = jnp.where(index == n - 1, 1, 0)
            for t in (turn, 1 - turn):
                target = dict(up)
                target[axis] = lax.rem(index + n - 1 + 2 * t, n)
                outgoing.append((axis, slot + t, target))
            groups[axis] = [(slot, (d,)), (slot + 1, (d + 4,))]
            slot += 2
    far, near = groups["ta"], groups["xy"] + groups["gz"]
    sends = []

    def send_chunk(rnd, src, y, axes=("ta", "xy", "gz")):
        for axis, s, target in outgoing:
            if axis not in axes:
                continue
            c = pltpu.make_async_remote_copy(
                src_ref=src.at[y], dst_ref=halos.at[rnd, s, y],
                send_sem=halo_send.at[rnd, s, y], recv_sem=halo_recv.at[rnd, s, y],
                device_id=target, device_id_type=MESH,
            )
            c.start()
            sends.append(c)

    def arrived(rnd, s, y):
        pltpu.make_async_remote_copy(
            src_ref=v_ref.at[y], dst_ref=halos.at[rnd, s, y],
            send_sem=halo_send.at[rnd, s, y], recv_sem=halo_recv.at[rnd, s, y],
            device_id=outgoing[0][2], device_id_type=MESH,
        ).wait_recv()

    def share(buf, mine, n, peer, send, recv):
        out = []
        for k in range(1, n):
            c = pltpu.make_async_remote_copy(
                src_ref=buf.at[mine], dst_ref=buf.at[mine],
                send_sem=send.at[k], recv_sem=recv.at[k],
                device_id=peer(k)[1], device_id_type=MESH,
            )
            c.start()
            out.append(c)
        sends.extend(out)
        return out

    def recv_all(copies):
        for c in copies:
            c.wait_recv()

    def add_slots(buf, n):
        parts = [buf[p] for p in range(n)]
        while len(parts) > 1:
            odd = parts[len(parts) // 2 * 2 :]
            parts = [a + b for a, b in zip(parts[::2], parts[1::2])] + odd
        return parts[0]

    lane = lax.broadcasted_iota(jnp.int32, (1, lanes), 1)
    low = lane < half
    jsign = jnp.where(low, -1.0, 1.0).astype(F32)

    def swap(x):
        return pltpu.roll(x, half, 1)

    def real(c):
        return jnp.where(low, c, swap(c))

    def imag(c):
        return jnp.where(low, swap(c), c)

    def factor(c):
        return real(c), imag(c) * jsign

    def times(f, x):
        return f[0] * x + f[1] * swap(x)

    def mul(a, b):
        return times(factor(a), b)

    def conj(a):
        return -jsign * a

    one = jnp.where(low, 1.0, 0.0).astype(F32)

    loads[0].wait()
    pl.semaphore_wait(barrier, len(greeted))
    for y in range(ny):
        send_chunk(0, v_ref, y, ("ta",))
    loads[1].wait()
    rows = pair(v_ref[...].reshape(ny * dof, lanes))
    cross = lax.dot_general(
        rows, pair(rhs_ref[...].reshape(ny * dof, lanes)), (((0,), (0,)), ((), ())),
        preferred_element_type=F32,
    )
    cross = cross[:lanes, :lanes] + (cross[:lanes, lanes:] + cross[lanes:, :lanes])
    corr = cross[:half] - jsign * swap(cross[half:])
    for p in range(plane):
        cpart[p] = corr[p * part : (p + 1) * part]
    rs_copies = []
    for k in range(1, plane):
        p, target = plane_peer(k)
        c = pltpu.make_async_remote_copy(
            src_ref=cpart.at[p], dst_ref=rs_buf.at[me],
            send_sem=rs_send.at[k], recv_sem=rs_recv.at[k],
            device_id=target, device_id_type=MESH,
        )
        c.start()
        rs_copies.append(c)
    rs_buf[me] = cpart[me]
    sends += rs_copies
    for y in range(ny):
        send_chunk(0, v_ref, y, ("xy", "gz"))
    for y in range(AHEAD):
        send_chunk(1, rhs_ref, y)

    loads[3].wait()
    loads[4].wait()
    theta = half / jnp.sum(er_ref[...], axis=1, keepdims=True)
    eye = lax.broadcasted_iota(jnp.int32, (half, half), 0) == lax.broadcasted_iota(
        jnp.int32, (half, half), 1
    )
    er = jnp.sum(jnp.where(eye, er_ref[...], 0.0), axis=1, keepdims=True)
    ei = jnp.sum(jnp.where(eye, ei_ref[...], 0.0), axis=1, keepdims=True)
    scale = 1.0 / (er * er + ei * ei)
    ec[0] = er * scale + jnp.zeros((half, lanes), F32)
    ec[1] = -jsign * (ei * scale)

    loads[2].wait()
    two = 2 * dof
    valid = lane < two

    def pick(ds, b, j):
        at = j * two
        base, off = (at // 128) * 128, at % 128
        start = pl.multiple_of(b * (4 * two), 128) + base
        width = 128 if off + two <= 128 else 256
        x = [links[d, :, pl.ds(start, width)] for d in ds]
        x = jnp.concatenate(x, 0) if len(x) > 1 else x[0]
        if off:
            x = pltpu.roll(x, width - off, 1)
        return jnp.where(valid, x[:, :128], 0.0)

    def relayout(b, carry):
        for ds in ((0, 1), (2, 3), (4, 5), (6, 7), (8,)):
            for j in range(4):
                row = ds[0] * ny * dof + 4 * b + j
                flat[pl.ds(row, len(ds) * ny, stride=dof), :] = pick(ds, b, j)
        return carry

    lax.fori_loop(0, dof // 4, relayout, 0)

    def direction(y, d):
        return flat[pl.ds((d * ny + y) * dof, dof), :]

    local_group = [(0,), (4,), (8,)]
    near_group = [ds for _, ds in near]
    far_group = [ds for _, ds in far]
    widths = [pad_to(len(g) * dof, 128) for g in (local_group, near_group, far_group)]
    bases = [0, widths[0], widths[0] + widths[1]]
    first_half = lane < dof
    diag = jnp.where(
        lax.broadcasted_iota(jnp.int32, (dof, lanes), 0)
        == lax.broadcasted_iota(jnp.int32, (dof, lanes), 1), 1.0, 0.0,
    )

    def place(parts, width):
        tiles = [jnp.zeros((dof, 128), F32)] * (width // 128)
        for m, p in enumerate(parts):
            t, w = divmod(dof * m, 128)
            r = pltpu.roll(p, w, 1) if w else p
            if w + dof <= 128:
                tiles[t] = tiles[t] + r
            else:
                tiles[t] = tiles[t] + jnp.where(lane >= w, r, 0.0)
                tiles[t + 1] = tiles[t + 1] + jnp.where(lane < w, r, 0.0)
        return jnp.concatenate(tiles, 1)

    def build(y):
        for g, group in enumerate((local_group, near_group, far_group)):
            res, ims = [], []
            for ds in group:
                x = direction(y, ds[0])
                for d in ds[1:]:
                    x = x + direction(y, d)
                x = x * theta
                if not ds[0]:
                    x = diag - x
                res.append(jnp.where(first_half, x, 0.0))
                ims.append(jnp.where(first_half, pltpu.roll(x, 128 - dof, 1), 0.0))
            for h, parts in enumerate((res, ims)):
                for i, piece in enumerate(split(place(parts, widths[g]))):
                    row = (2 * i + h) * dof
                    mats[y, row : row + dof, bases[g] : bases[g] + widths[g]] = piece

    def product(y, g, blocks):
        width = widths[g]
        rest = width - len(blocks) * dof
        if rest:
            blocks = blocks + [jnp.zeros((rest, 2 * lanes), BF16)]
        out = jnp.dot(
            mats[y, :, bases[g] : bases[g] + width], jnp.concatenate(blocks, 0),
            preferred_element_type=F32,
        )
        return out[:two, :lanes] + (out[:two, lanes:] + out[two:, :lanes])

    def begin():
        for y in range(ny):
            acc[y] = product(y, 0, [pcs[y], pcs[(y + 1) % ny], pcs[(y - 1) % ny]])

    def halo_blocks(rnd, y, group):
        blocks = []
        for s, _ in group:
            arrived(rnd, s, y)
            blocks.append(pair(halos[rnd, s, y]))
        return blocks

    def middle(rnd, y):
        acc[y] += product(y, 1, halo_blocks(rnd, y, near))

    def finish(rnd, y):
        t = acc[y] + product(y, 2, halo_blocks(rnd, y, far))
        return t[:dof] + jsign * swap(t[dof:])

    recv_all(rs_copies)
    ct_buf[it] = add_slots(rs_buf, plane)
    ct_copies = share(ct_buf, it, nt, time_peer, ct_send, ct_recv)
    for y in range(AHEAD, ny):
        send_chunk(1, rhs_ref, y)

    for y in range(ny):
        build(y)
    for y in range(ny):
        pcs[y] = pair(v_ref[y])
    begin()

    inverse = 1.0 / theta
    for y in range(ny):
        middle(0, y)
    recv_all(ct_copies)
    total = add_slots(ct_buf, nt)
    mine = pl.ds(me * part, part)
    ag_buf[me] = total * ec[0, mine] + swap(total) * ec[1, mine]
    ag_copies = share(ag_buf, me, plane, plane_peer, ag_send, ag_recv)

    for y in range(ny):
        v = v_ref[y]
        w = (v - finish(0, y)) * inverse
        image_ref[y] = w
        send_chunk(2, image_ref, y)
        for i, piece in enumerate(split(w) + split(v)):
            vw[y, i * dof : (i + 1) * dof] = piece
    for y in range(ny):
        pcs[y] = pair(rhs_ref[y])
    begin()
    for y in range(ny):
        middle(1, y)

    for y in range(ny):
        fields[1, y] = finish(1, y)
    for y in range(ny):
        pcs[y] = pair(image_ref[y])
    begin()
    for y in range(ny):
        middle(2, y)

    recv_all(ag_copies)
    coef = jnp.concatenate([ag_buf[p] for p in range(plane)], 0)
    block = pair(jnp.concatenate([coef, jsign * swap(coef)], 0))

    def expand(left):
        out = jnp.dot(left, block, preferred_element_type=F32)
        return out[:dof, :lanes] + (out[:dof, lanes:] + out[dof:, :lanes])

    for y in range(ny):
        r = fields[1, y] - expand(jnp.concatenate(split(finish(2, y)), 0))
        fields[1, y] = r
        send_chunk(3, fields.at[1], y)
        pcs[y] = pair(r)
    for y in range(ny):
        fields[0, y] = rhs_ref[y] - expand(vw[y, :two])
        start_ref[y] = expand(vw[y, two:])

    def fold(x):
        return jnp.sum(x.reshape(dof // 8, 8, lanes), axis=0)

    def partials(x0, x1, x2):
        u0, u1 = x0 - x1, x1 - x2
        s0, t0 = swap(x0), swap(u0)
        return [
            fold(p)
            for p in (u0 * x0, u0 * s0, u1 * x0, u1 * s0, u1 * u0, u1 * t0, u0 * u0, u1 * u1)
        ]

    def add(a, b):
        return b if a is None else [p + q for p, q in zip(a, b)]

    def gram(sums):
        s = [jnp.sum(p, axis=0, keepdims=True) for p in sums]
        out = [
            jnp.where(low, s[i] + swap(s[i]), swap(s[i + 1]) - s[i + 1]) for i in (0, 2, 4)
        ]
        out.append(jnp.where(low, s[6] + swap(s[6]), s[7] + swap(s[7])))
        row = lax.broadcasted_iota(jnp.int32, (4, lanes), 0)
        x = out[3]
        for i in (2, 1, 0):
            x = jnp.where(row == i, out[i], x)
        return x

    def steps(total):
        a, b, c, d = (total[i : i + 1] for i in range(4))
        b0 = a / real(d)
        e = mul(conj(b0), c)
        num = mul(conj(b0), b) - mul(real(mul(conj(b0), b0)) * one, c)
        near_one = one - b0
        size0 = real(mul(conj(near_one), near_one))
        size1 = real(mul(conj(b0), b0))
        den = size0 * real(d) + size1 * imag(d) + 2.0 * real(mul(near_one, e))
        b1 = num / den
        both = mul(b0, b1)
        mixed = b0 + b1 - both
        poly = [factor(x) for x in (one - mixed, mixed - both, both)]
        gain = [factor(theta * x) for x in (mixed, both)]
        return poly, gain

    def combine(poly, xs):
        out = times(poly[0], xs[0])
        for p, x in zip(poly[1:], xs[1:]):
            out = out + times(p, x)
        return out

    def step(rnd, y):
        out = finish(rnd, y)
        fields[rnd - 1, y] = out
        if rnd < rounds - 1:
            send_chunk(rnd + 1, fields.at[rnd - 1], y)
            pcs[y] = pair(out)

    poly = gain = None
    sums = None
    rounds = SWEEPS + 2
    for rnd in range(3, rounds):
        begin()
        if rnd == 4:
            for y in range(ny):
                sums = add(sums, partials(fields[0, y], fields[1, y], fields[2, y]))
            st_buf[0, it] = gram(sums)
            early = share(st_buf.at[0], it, nt, time_peer, st_send.at[0], st_recv.at[0])
        if rnd == 5:
            recv_all(early)
            sp_buf[0, me] = add_slots(st_buf.at[0], nt)
            early = share(sp_buf.at[0], me, plane, plane_peer, sp_send.at[0], sp_recv.at[0])
        for y in range(ny + LEAD):
            if y < ny:
                middle(rnd, y)
            if y >= LEAD:
                step(rnd, y - LEAD)
    recv_all(early)
    poly, gain = steps(add_slots(sp_buf.at[0], plane))
    sums = None
    for y in range(ny):
        f = [fields[i, y] for i in range(SWEEPS + 1)]
        g = [combine(poly, f[i : i + 3]) for i in range(3)]
        for i in range(3):
            g_ref[i, y] = g[i]
        start_ref[y] = start_ref[y] + combine(gain, f[:2])
        sums = add(sums, partials(*g))
    if direct:
        sd_buf[rank] = gram(sums)
        last = share(sd_buf, rank, everyone, any_peer, sd_send, sd_recv)
        recv_all(last)
        total = add_slots(sd_buf, everyone)
    else:
        st_buf[1, it] = gram(sums)
        last = share(st_buf.at[1], it, nt, time_peer, st_send.at[1], st_recv.at[1])
        recv_all(last)
        sp_buf[1, me] = add_slots(st_buf.at[1], nt)
        last = share(sp_buf.at[1], me, plane, plane_peer, sp_send.at[1], sp_recv.at[1])
        recv_all(last)
        total = add_slots(sp_buf.at[1], plane)
    poly, gain = steps(total)
    for y in range(ny):
        g = [g_ref[i, y] for i in range(3)]
        sol_ref[y] = start_ref[y] + combine(gain, g[:2])
        res_ref[y] = combine(poly, g)
    for c in sends:
        c.wait_send()


def hand_over(a_ref, b_ref, sol_ref, res_ref):
    sol_ref[...] = a_ref[...]
    res_ref[...] = b_ref[...]


def local(sizes, links, eigvecs, eig_real, eig_imag, rhs):
    nt, nz, nx = sizes
    plane = nz * nx
    ny, dof, lanes = rhs.shape[3:]
    half = lanes // 2
    field = (ny, dof, lanes)
    ndir = links.shape[4]
    slots = sum(1 if n == 2 else 2 for n in sizes)
    far = 1 if nt == 2 else 2
    part = half // plane
    rounds = SWEEPS + 2
    everyone = nt * plane
    direct = everyone if everyone <= DIRECT else 1
    width = sum(pad_to(n * dof, 128) for n in (3, slots - far, far))
    vmem, dma = pltpu.VMEM, pltpu.SemaphoreType.DMA
    spec = pl.BlockSpec(memory_space=pltpu.VMEM)
    sol, res = pl.pallas_call(
        functools.partial(kernel, sizes, field),
        out_shape=[vmem(field, F32)] * 2,
        in_specs=[pl.BlockSpec(memory_space=pl.ANY)] * 5,
        out_specs=[spec] * 2,
        scratch_shapes=[
            vmem((ndir, ny, links.shape[5]), F32),
            vmem(field, F32),
            vmem(field, F32),
            vmem((1, half), F32),
            vmem((1, half), F32),
            vmem((ndir * ny * dof, 128), F32),
            vmem((ny, 4 * dof, width), BF16),
            vmem((ny, 2 * dof, lanes), F32),
            vmem((ny, dof, 2 * lanes), BF16),
            vmem((SWEEPS + 1,) + field, F32),
            vmem((rounds, slots) + field, F32),
            vmem((ny, 4 * dof, lanes), BF16),
            vmem(field, F32),
            vmem(field, F32),
            vmem((3,) + field, F32),
            vmem((plane, part, lanes), F32),
            vmem((plane, part, lanes), F32),
            vmem((nt, part, lanes), F32),
            vmem((plane, part, lanes), F32),
            vmem((2, half, lanes), F32),
            vmem((2, nt, 4, lanes), F32),
            vmem((2, plane, 4, lanes), F32),
            vmem((direct, 4, lanes), F32),
            dma((5,)),
            dma((rounds, slots, ny)),
            dma((rounds, slots, ny)),
            dma((plane,)),
            dma((plane,)),
            dma((nt,)),
            dma((nt,)),
            dma((plane,)),
            dma((plane,)),
            dma((2, nt)),
            dma((2, nt)),
            dma((2, plane)),
            dma((2, plane)),
            dma((direct,)),
            dma((direct,)),
        ],
        compiler_params=pltpu.CompilerParams(collective_id=0, has_side_effects=True),
    )(
        links.reshape(links.shape[3:]).transpose(1, 0, 2),
        eigvecs.reshape(field),
        eig_real.reshape(1, -1),
        eig_imag.reshape(1, -1),
        rhs.reshape(field),
    )
    sol, res = pl.pallas_call(
        hand_over,
        out_shape=[jax.ShapeDtypeStruct(field, F32)] * 2,
        in_specs=[spec] * 2,
        out_specs=[spec] * 2,
    )(*(pltpu.with_memory_space_constraint(x, pltpu.VMEM) for x in (sol, res)))
    return (sol.reshape(rhs.shape), res.reshape(rhs.shape))


def solution(mesh):
    whole = P("ta", "gz", "xy", None, None, None)
    sizes = tuple(mesh.shape[a] for a in ("ta", "gz", "xy"))
    return jax.shard_map(
        functools.partial(local, sizes),
        mesh=mesh,
        in_specs=(whole, whole, P(), P(), whole),
        out_specs=(whole, whole),
        check_vma=False,
    )
```

```python
import functools

import jax
import jax.numpy as jnp
from jax import lax
from jax.experimental import pallas as pl
from jax.experimental.pallas import tpu as pltpu
from jax.sharding import PartitionSpec as P

SWEEPS = 4
LEAD = 0
LAG = 5
EARLY = 2
DIRECT = 32
MESH = pl.DeviceIdType.MESH
F32, BF16 = jnp.float32, jnp.bfloat16


def split(x):
    first = x.astype(BF16)
    return first, (x - first.astype(F32)).astype(BF16)


def pair(x):
    return jnp.concatenate(split(x), 1)


def pad_to(n, m):
    return -(-n // m) * m


def kernel(
    sizes, dims, links_hbm, v_hbm, er_hbm, ei_hbm, rhs_hbm, sol_ref, res_ref,
    links, v_ref, rhs_ref, er_ref, ei_ref, flat, mats, acc, pcs, fields, halos, vw, image_ref, start_ref,
    g_ref, cpart, rs_buf, ct_buf, ag_buf, ec, st_buf, sp_buf, sd_buf,
    in_sem, halo_send, halo_recv, rs_send, rs_recv, ct_send, ct_recv, ag_send, ag_recv,
    st_send, st_recv, sp_send, sp_recv, sd_send, sd_recv,
):
    nt, nz, nx = sizes
    ny, dof, lanes = dims
    half = lanes // 2
    plane = nz * nx
    it, iz, ix = lax.axis_index("ta"), lax.axis_index("gz"), lax.axis_index("xy")
    me = iz * nx + ix
    part = half // plane

    def ranked(*ns):
        steps = [()]
        for n in ns:
            steps = [o + (d,) for o in steps for d in range(n)]
        steps.sort(key=lambda o: -sum(min(d, n - d) for d, n in zip(o, ns)))
        return steps[-1:] + steps[:-1]

    plane_steps, all_steps = ranked(nz, nx), ranked(nt, nz, nx)

    def plane_peer(k):
        dz, dx = plane_steps[k]
        z, x = lax.rem(iz + dz, nz), lax.rem(ix + dx, nx)
        return z * nx + x, {"ta": it, "gz": z, "xy": x}

    def time_peer(k):
        p = lax.rem(it + k, nt)
        return p, {"ta": p, "gz": iz, "xy": ix}

    everyone = nt * plane
    rank = it * plane + me

    def any_peer(k):
        dt, dz, dx = all_steps[k]
        t, z, x = lax.rem(it + dt, nt), lax.rem(iz + dz, nz), lax.rem(ix + dx, nx)
        return t * plane + z * nx + x, {"ta": t, "gz": z, "xy": x}

    direct = everyone <= DIRECT
    greeted = [plane_peer(k)[1] for k in range(1, plane)]
    greeted += [time_peer(k)[1] for k in range(1, nt)]
    barrier = pltpu.get_barrier_semaphore()
    for target in greeted:
        pl.semaphore_signal(barrier, inc=1, device_id=target, device_id_type=MESH)

    loads = []
    for i, (src, dst) in enumerate(
        ((v_hbm, v_ref), (rhs_hbm, rhs_ref), (links_hbm, links), (er_hbm, er_ref), (ei_hbm, ei_ref))
    ):
        c = pltpu.make_async_copy(src, dst, in_sem.at[i])
        c.start()
        loads.append(c)

    def neighbours(axis, index, n):
        base = {"ta": it, "gz": iz, "xy": ix}
        up, down = dict(base), dict(base)
        up[axis] = lax.rem(index + 1, n)
        down[axis] = lax.rem(index + n - 1, n)
        return up, down

    outgoing, groups, slot = [], {}, 0
    for axis, index, n, d in (("ta", it, nt, 1), ("xy", ix, nx, 3), ("gz", iz, nz, 2)):
        up, down = neighbours(axis, index, n)
        if n == 2:
            outgoing.append((axis, slot, up))
            groups[axis] = [(slot, (d, d + 4))]
            slot += 1
        else:
            turn = jnp.where(index == n - 1, 1, 0)
            for t in (turn, 1 - turn):
                target = dict(up)
                target[axis] = lax.rem(index + n - 1 + 2 * t, n)
                outgoing.append((axis, slot + t, target))
            groups[axis] = [(slot, (d,)), (slot + 1, (d + 4,))]
            slot += 2
    far, near = groups["ta"], groups["xy"] + groups["gz"]
    sends = []

    def send_to(rnd, src, y, targets):
        for axis, s, target in targets:
            c = pltpu.make_async_remote_copy(
                src_ref=src.at[y], dst_ref=halos.at[rnd, s, y],
                send_sem=halo_send.at[rnd, s, y], recv_sem=halo_recv.at[rnd, s, y],
                device_id=target, device_id_type=MESH,
            )
            c.start()
            sends.append(c)

    first_far, second_far = outgoing[:1], outgoing[1 : len(far)]
    beside = outgoing[len(far) :]

    def send_far(rnd, src, y):
        send_to(rnd, src, y, first_far)
        if rnd == LAG:
            if y:
                send_to(rnd, src, y - 1, second_far)
            if y == ny - 1:
                send_to(rnd, src, y, second_far)
        else:
            send_to(rnd, src, y, second_far)

    def send_chunk(rnd, src, y):
        send_far(rnd, src, y)
        send_to(rnd, src, y, beside)

    def arrived(rnd, s, y):
        pltpu.make_async_remote_copy(
            src_ref=v_ref.at[y], dst_ref=halos.at[rnd, s, y],
            send_sem=halo_send.at[rnd, s, y], recv_sem=halo_recv.at[rnd, s, y],
            device_id=outgoing[0][2], device_id_type=MESH,
        ).wait_recv()

    def share(buf, mine, n, peer, send, recv):
        out = []
        for k in range(1, n):
            c = pltpu.make_async_remote_copy(
                src_ref=buf.at[mine], dst_ref=buf.at[mine],
                send_sem=send.at[k], recv_sem=recv.at[k],
                device_id=peer(k)[1], device_id_type=MESH,
            )
            c.start()
            out.append(c)
        sends.extend(out)
        return out

    def recv_all(copies):
        for c in copies:
            c.wait_recv()

    def add_slots(buf, n):
        parts = [buf[p] for p in range(n)]
        while len(parts) > 1:
            odd = parts[len(parts) // 2 * 2 :]
            parts = [a + b for a, b in zip(parts[::2], parts[1::2])] + odd
        return parts[0]

    lane = lax.broadcasted_iota(jnp.int32, (1, lanes), 1)
    low = lane < half
    jsign = jnp.where(low, -1.0, 1.0).astype(F32)

    def swap(x):
        return pltpu.roll(x, half, 1)

    def real(c):
        return jnp.where(low, c, swap(c))

    def imag(c):
        return jnp.where(low, swap(c), c)

    def times(f, x):
        return f[0] * x + f[1] * swap(x)

    loads[0].wait()
    pl.semaphore_wait(barrier, len(greeted))
    for y in range(ny):
        send_far(0, v_ref, y)
    loads[1].wait()
    rows = pair(v_ref[...].reshape(ny * dof, lanes))
    cross = lax.dot_general(
        rows, pair(rhs_ref[...].reshape(ny * dof, lanes)), (((0,), (0,)), ((), ())),
        preferred_element_type=F32,
    )
    cross = cross[:lanes, :lanes] + (cross[:lanes, lanes:] + cross[lanes:, :lanes])
    corr = cross[:half] - jsign * swap(cross[half:])
    for p in range(plane):
        cpart[p] = corr[p * part : (p + 1) * part]
    rs_copies = []
    for k in range(1, plane):
        p, target = plane_peer(k)
        c = pltpu.make_async_remote_copy(
            src_ref=cpart.at[p], dst_ref=rs_buf.at[me],
            send_sem=rs_send.at[k], recv_sem=rs_recv.at[k],
            device_id=target, device_id_type=MESH,
        )
        c.start()
        rs_copies.append(c)
    rs_buf[me] = cpart[me]
    sends += rs_copies
    for y in range(ny):
        send_to(0, v_ref, y, beside)

    loads[3].wait()
    loads[4].wait()
    theta = half / jnp.sum(er_ref[...], axis=1, keepdims=True)
    eye = lax.broadcasted_iota(jnp.int32, (half, half), 0) == lax.broadcasted_iota(
        jnp.int32, (half, half), 1
    )
    er = jnp.sum(jnp.where(eye, er_ref[...], 0.0), axis=1, keepdims=True)
    ei = jnp.sum(jnp.where(eye, ei_ref[...], 0.0), axis=1, keepdims=True)
    scale = 1.0 / (er * er + ei * ei)
    ec[0] = er * scale + jnp.zeros((half, lanes), F32)
    ec[1] = -jsign * (ei * scale)

    loads[2].wait()
    two = 2 * dof
    valid = lane < two

    def pick(ds, b, j):
        at = j * two
        base, off = (at // 128) * 128, at % 128
        start = pl.multiple_of(b * (4 * two), 128) + base
        width = 128 if off + two <= 128 else 256
        x = [links[d, :, pl.ds(start, width)] for d in ds]
        x = jnp.concatenate(x, 0) if len(x) > 1 else x[0]
        if off:
            x = pltpu.roll(x, width - off, 1)
        return jnp.where(valid, x[:, :128], 0.0)

    def relayout(b, carry):
        for ds in ((0, 1), (2, 3), (4, 5), (6, 7), (8,)):
            for j in range(4):
                row = ds[0] * ny * dof + 4 * b + j
                flat[pl.ds(row, len(ds) * ny, stride=dof), :] = pick(ds, b, j)
        return carry

    lax.fori_loop(0, dof // 4, relayout, 0)

    def direction(y, d):
        return flat[pl.ds((d * ny + y) * dof, dof), :]

    local_group = [(0,), (4,), (8,)]
    near_group = [ds for _, ds in near]
    far_group = [ds for _, ds in far]
    widths = [pad_to(len(g) * dof, 128) for g in (local_group, near_group, far_group)]
    bases = [0, widths[0], widths[0] + widths[1]]
    first_half = lane < dof
    diag = jnp.where(
        lax.broadcasted_iota(jnp.int32, (dof, lanes), 0)
        == lax.broadcasted_iota(jnp.int32, (dof, lanes), 1), 1.0, 0.0,
    )

    def place(parts, width):
        tiles = [jnp.zeros((dof, 128), F32)] * (width // 128)
        for m, p in enumerate(parts):
            t, w = divmod(dof * m, 128)
            r = pltpu.roll(p, w, 1) if w else p
            if w + dof <= 128:
                tiles[t] = tiles[t] + r
            else:
                tiles[t] = tiles[t] + jnp.where(lane >= w, r, 0.0)
                tiles[t + 1] = tiles[t + 1] + jnp.where(lane < w, r, 0.0)
        return jnp.concatenate(tiles, 1)

    def build(y):
        for g, group in enumerate((local_group, near_group, far_group)):
            res, ims = [], []
            for ds in group:
                x = direction(y, ds[0])
                for d in ds[1:]:
                    x = x + direction(y, d)
                x = x * theta
                if not ds[0]:
                    x = diag - x
                res.append(jnp.where(first_half, x, 0.0))
                ims.append(jnp.where(first_half, pltpu.roll(x, 128 - dof, 1), 0.0))
            for h, parts in enumerate((res, ims)):
                for i, piece in enumerate(split(place(parts, widths[g]))):
                    row = (2 * i + h) * dof
                    mats[y, row : row + dof, bases[g] : bases[g] + widths[g]] = piece

    def product(y, g, blocks):
        width = widths[g]
        rest = width - len(blocks) * dof
        if rest:
            blocks = blocks + [jnp.zeros((rest, 2 * lanes), BF16)]
        out = jnp.dot(
            mats[y, :, bases[g] : bases[g] + width], jnp.concatenate(blocks, 0),
            preferred_element_type=F32,
        )
        return out[:two, :lanes] + (out[:two, lanes:] + out[two:, :lanes])

    def begin(a=0):
        for y in range(ny):
            acc[a, y] = product(y, 0, [pcs[y], pcs[(y + 1) % ny], pcs[(y - 1) % ny]])

    def halo_blocks(rnd, y, group):
        blocks = []
        for s, _ in group:
            arrived(rnd, s, y)
            blocks.append(pair(halos[rnd, s, y]))
        return blocks

    def middle(rnd, y, a=0):
        acc[a, y] += product(y, 1, halo_blocks(rnd, y, near))

    def finish(rnd, y, a=0):
        t = acc[a, y] + product(y, 2, halo_blocks(rnd, y, far))
        return t[:dof] + jsign * swap(t[dof:])

    recv_all(rs_copies)
    ct_buf[it] = add_slots(rs_buf, plane)
    ct_copies = share(ct_buf, it, nt, time_peer, ct_send, ct_recv)
    for y in range(EARLY):
        send_far(1, rhs_ref, y)
    for y in range(ny):
        send_to(1, rhs_ref, y, beside)

    for y in range(ny):
        build(y)
    for y in range(ny):
        pcs[y] = pair(v_ref[y])
    begin()

    inverse = 1.0 / theta
    for y in range(ny):
        middle(0, y)
    for y in range(ny):
        v = v_ref[y]
        w = (v - finish(0, y)) * inverse
        image_ref[y] = w
        send_far(2, image_ref, y)
        if y + EARLY < ny:
            send_far(1, rhs_ref, y + EARLY)
        for i, piece in enumerate(split(w) + split(v)):
            vw[y, i * dof : (i + 1) * dof] = piece
    recv_all(ct_copies)
    total = add_slots(ct_buf, nt)
    mine = pl.ds(me * part, part)
    ag_buf[me] = total * ec[0, mine] + swap(total) * ec[1, mine]
    ag_copies = share(ag_buf, me, plane, plane_peer, ag_send, ag_recv)
    for y in range(ny):
        send_to(2, image_ref, y, beside)
    for y in range(ny):
        pcs[y] = pair(rhs_ref[y])
    begin()
    for y in range(ny):
        middle(1, y)

    for y in range(ny):
        pcs[y] = pair(image_ref[y])
    begin(1)
    for y in range(ny):
        middle(2, y, 1)

    recv_all(ag_copies)
    coef = jnp.concatenate([ag_buf[p] for p in range(plane)], 0)
    block = pair(jnp.concatenate([coef, jsign * swap(coef)], 0))

    def expand(left):
        out = jnp.dot(left, block, preferred_element_type=F32)
        return out[:dof, :lanes] + (out[:dof, lanes:] + out[dof:, :lanes])

    for y in range(ny):
        r = finish(1, y) - expand(jnp.concatenate(split(finish(2, y, 1)), 0))
        fields[1, y] = r
        send_chunk(3, fields.at[1], y)
        pcs[y] = pair(r)
    for y in range(ny):
        fields[0, y] = rhs_ref[y] - expand(vw[y, :two])
        start_ref[y] = expand(vw[y, two:])

    def fold(x):
        return jnp.sum(x.reshape(dof // 8, 8, lanes), axis=0)

    def partials(x0, x1, x2):
        u0, u1 = x0 - x1, x1 - x2
        s0, t0 = swap(x0), swap(u0)
        return [
            fold(p)
            for p in (u0 * x0, u1 * x0, u1 * u0, u0 * u0, u0 * s0, u1 * s0, u1 * t0, u1 * u1)
        ]

    def add(a, b):
        return b if a is None else [p + q for p, q in zip(a, b)]

    def gram(sums):
        row = lax.broadcasted_iota(jnp.int32, (8, lanes), 0)
        x = jnp.sum(sums[7], axis=0, keepdims=True)
        for i in range(7):
            x = jnp.where(row == i, jnp.sum(sums[i], axis=0, keepdims=True), x)
        r = swap(x)
        y = r + jnp.where((row < 4) | (row == 7), x, -x)
        return jnp.where(low, y[:4], y[4:])

    def product_of(x, y):
        return x[0] * y[0] - x[1] * y[1], x[0] * y[1] + x[1] * y[0]

    def inner(x, y):
        return x[0] * y[0] + x[1] * y[1], x[0] * y[1] - x[1] * y[0]

    def steps(total):
        r, i = real(total), imag(total)
        a, b, c = ((r[k : k + 1], i[k : k + 1]) for k in range(3))
        size, other = r[3:4], i[3:4]
        b0 = (a[0] / size, a[1] / size)
        power = b0[0] * b0[0] + b0[1] * b0[1]
        num = inner(b0, b)
        num = (num[0] - power * c[0], num[1] - power * c[1])
        left = (1.0 - b0[0], -b0[1])
        e = product_of(left, inner(b0, c))
        den = (left[0] * left[0] + left[1] * left[1]) * size + power * other + 2.0 * e[0]
        b1 = (num[0] / den, num[1] / den)
        both = product_of(b0, b1)
        mixed = tuple(p + q - t for p, q, t in zip(b0, b1, both))
        poly = ((1.0 - mixed[0], -mixed[1]), tuple(p - q for p, q in zip(mixed, both)), both)
        poly = [(p, q * jsign) for p, q in poly]
        gain = [(theta * p, theta * q * jsign) for p, q in (mixed, both)]
        return poly, gain

    def combine(poly, xs):
        out = times(poly[0], xs[0])
        for p, x in zip(poly[1:], xs[1:]):
            out = out + times(p, x)
        return out

    def step(rnd, y):
        out = finish(rnd, y)
        fields[rnd - 1, y] = out
        if rnd < rounds - 1:
            send_chunk(rnd + 1, fields.at[rnd - 1], y)
            pcs[y] = pair(out)

    poly = gain = None
    sums = None
    rounds = SWEEPS + 2
    for rnd in range(3, rounds):
        begin()
        if rnd == 4:
            for y in range(ny):
                sums = add(sums, partials(fields[0, y], fields[1, y], fields[2, y]))
            st_buf[0, it] = gram(sums)
            early = share(st_buf.at[0], it, nt, time_peer, st_send.at[0], st_recv.at[0])
        if rnd == 5:
            recv_all(early)
            sp_buf[0, me] = add_slots(st_buf.at[0], nt)
            early = share(sp_buf.at[0], me, plane, plane_peer, sp_send.at[0], sp_recv.at[0])
        for y in range(ny + LEAD):
            if y < ny:
                middle(rnd, y)
            if y >= LEAD:
                step(rnd, y - LEAD)
    recv_all(early)
    poly, gain = steps(add_slots(sp_buf.at[0], plane))
    sums = None
    for y in range(ny):
        f = [fields[i, y] for i in range(SWEEPS + 1)]
        g = [combine(poly, f[i : i + 3]) for i in range(3)]
        for i in range(3):
            g_ref[2 * i, y] = g[i]
            g_ref[2 * i + 1, y] = swap(g[i])
        start_ref[y] = start_ref[y] + combine(gain, f[:2])
        sums = add(sums, partials(*g))
    def drain():
        for c in sends:
            c.wait_send()

    if direct:
        sd_buf[rank] = gram(sums)
        last = share(sd_buf, rank, everyone, any_peer, sd_send, sd_recv)
        drain()
        recv_all(last)
        total = add_slots(sd_buf, everyone)
    else:
        st_buf[1, it] = gram(sums)
        last = share(st_buf.at[1], it, nt, time_peer, st_send.at[1], st_recv.at[1])
        recv_all(last)
        sp_buf[1, me] = add_slots(st_buf.at[1], nt)
        last = share(sp_buf.at[1], me, plane, plane_peer, sp_send.at[1], sp_recv.at[1])
        drain()
        recv_all(last)
        total = add_slots(sp_buf.at[1], plane)
    poly, gain = steps(total)
    def blend(f, y):
        out = f[0][0] * g_ref[0, y] + f[0][1] * g_ref[1, y]
        for i in range(1, len(f)):
            out = out + (f[i][0] * g_ref[2 * i, y] + f[i][1] * g_ref[2 * i + 1, y])
        return out

    for y in range(ny):
        sol_ref[y] = start_ref[y] + blend(gain, y)
        res_ref[y] = blend(poly, y)


def hand_over(a_ref, b_ref, sol_ref, res_ref):
    sol_ref[...] = a_ref[...]
    res_ref[...] = b_ref[...]


def local(sizes, links, eigvecs, eig_real, eig_imag, rhs):
    nt, nz, nx = sizes
    plane = nz * nx
    ny, dof, lanes = rhs.shape[3:]
    half = lanes // 2
    field = (ny, dof, lanes)
    ndir = links.shape[4]
    slots = sum(1 if n == 2 else 2 for n in sizes)
    far = 1 if nt == 2 else 2
    part = half // plane
    rounds = SWEEPS + 2
    everyone = nt * plane
    direct = everyone if everyone <= DIRECT else 1
    width = sum(pad_to(n * dof, 128) for n in (3, slots - far, far))
    vmem, dma = pltpu.VMEM, pltpu.SemaphoreType.DMA
    spec = pl.BlockSpec(memory_space=pltpu.VMEM)
    sol, res = pl.pallas_call(
        functools.partial(kernel, sizes, field),
        out_shape=[vmem(field, F32)] * 2,
        in_specs=[pl.BlockSpec(memory_space=pl.ANY)] * 5,
        out_specs=[spec] * 2,
        scratch_shapes=[
            vmem((ndir, ny, links.shape[5]), F32),
            vmem(field, F32),
            vmem(field, F32),
            vmem((1, half), F32),
            vmem((1, half), F32),
            vmem((ndir * ny * dof, 128), F32),
            vmem((ny, 4 * dof, width), BF16),
            vmem((2, ny, 2 * dof, lanes), F32),
            vmem((ny, dof, 2 * lanes), BF16),
            vmem((SWEEPS + 1,) + field, F32),
            vmem((rounds, slots) + field, F32),
            vmem((ny, 4 * dof, lanes), BF16),
            vmem(field, F32),
            vmem(field, F32),
            vmem((6,) + field, F32),
            vmem((plane, part, lanes), F32),
            vmem((plane, part, lanes), F32),
            vmem((nt, part, lanes), F32),
            vmem((plane, part, lanes), F32),
            vmem((2, half, lanes), F32),
            vmem((2, nt, 4, lanes), F32),
            vmem((2, plane, 4, lanes), F32),
            vmem((direct, 4, lanes), F32),
            dma((5,)),
            dma((rounds, slots, ny)),
            dma((rounds, slots, ny)),
            dma((plane,)),
            dma((plane,)),
            dma((nt,)),
            dma((nt,)),
            dma((plane,)),
            dma((plane,)),
            dma((2, nt)),
            dma((2, nt)),
            dma((2, plane)),
            dma((2, plane)),
            dma((direct,)),
            dma((direct,)),
        ],
        compiler_params=pltpu.CompilerParams(collective_id=0, has_side_effects=True),
    )(
        links.reshape(links.shape[3:]).transpose(1, 0, 2),
        eigvecs.reshape(field),
        eig_real.reshape(1, -1),
        eig_imag.reshape(1, -1),
        rhs.reshape(field),
    )
    sol, res = pl.pallas_call(
        hand_over,
        out_shape=[jax.ShapeDtypeStruct(field, F32)] * 2,
        in_specs=[spec] * 2,
        out_specs=[spec] * 2,
    )(*(pltpu.with_memory_space_constraint(x, pltpu.VMEM) for x in (sol, res)))
    return (sol.reshape(rhs.shape), res.reshape(rhs.shape))


def solution(mesh):
    whole = P("ta", "gz", "xy", None, None, None)
    sizes = tuple(mesh.shape[a] for a in ("ta", "gz", "xy"))
    return jax.shard_map(
        functools.partial(local, sizes),
        mesh=mesh,
        in_specs=(whole, whole, P(), P(), whole),
        out_specs=(whole, whole),
        check_vma=False,
    )
```

```python
import functools

import jax
import jax.numpy as jnp
from jax import lax
from jax.experimental import pallas as pl
from jax.experimental.pallas import tpu as pltpu
from jax.sharding import PartitionSpec as P

SWEEPS = 4
LEAD = 0
LAG = 5
EARLY = 2
DIRECT = 32
MESH = pl.DeviceIdType.MESH
F32, BF16 = jnp.float32, jnp.bfloat16


def split(x):
    first = x.astype(BF16)
    return first, (x - first.astype(F32)).astype(BF16)


def pair(x):
    return jnp.concatenate(split(x), 1)


def pad_to(n, m):
    return -(-n // m) * m


def kernel(
    sizes, dims, links_hbm, v_hbm, er_hbm, ei_hbm, rhs_hbm, sol_ref, res_ref,
    links, v_ref, rhs_ref, er_ref, ei_ref, flat, mats, acc, pcs, fields, halos, vw, image_ref, start_ref,
    g_ref, cpart, rs_buf, ct_buf, ag_buf, ec, st_buf, sp_buf, sd_buf,
    token, in_sem, halo_send, halo_recv, rs_send, rs_recv, ct_send, ct_recv, ag_send, ag_recv,
    st_send, st_recv, sp_send, sp_recv, sd_send, sd_recv,
):
    nt, nz, nx = sizes
    ny, dof, lanes = dims
    half = lanes // 2
    plane = nz * nx
    it, iz, ix = lax.axis_index("ta"), lax.axis_index("gz"), lax.axis_index("xy")
    me = iz * nx + ix
    part = half // plane

    def ranked(*ns):
        steps = [()]
        for n in ns:
            steps = [o + (d,) for o in steps for d in range(n)]
        steps.sort(key=lambda o: -sum(min(d, n - d) for d, n in zip(o, ns)))
        return steps[-1:] + steps[:-1]

    plane_steps = ranked(nz, nx)

    def plane_peer(k):
        dz, dx = plane_steps[k]
        z, x = lax.rem(iz + dz, nz), lax.rem(ix + dx, nx)
        return z * nx + x, {"ta": it, "gz": z, "xy": x}

    def time_peer(k):
        p = lax.rem(it + k, nt)
        return p, {"ta": p, "gz": iz, "xy": ix}

    everyone = nt * plane
    rank = it * plane + me

    def other(j):
        p = j + jnp.where(rank <= j, 1, 0)
        r = lax.rem(p, plane)
        return p, {"ta": lax.div(p, plane), "gz": lax.div(r, nx), "xy": lax.rem(r, nx)}

    direct = everyone <= DIRECT
    barrier = pltpu.get_barrier_semaphore()

    def at_time(p):
        return {"ta": p, "gz": iz, "xy": ix}

    def signal_when(test, sem, p):
        @pl.when(test)
        def _():
            pl.semaphore_signal(sem, inc=1, device_id=at_time(p), device_id_type=MESH)

    def wait_when(test, sem):
        @pl.when(test)
        def _():
            pl.semaphore_wait(sem, 1)

    above, below = it < nt - 1, it > 0
    signal_when(above, barrier, it + 1)
    signal_when(below, barrier, it - 1)
    for k in range(1, plane):
        pl.semaphore_signal(barrier, inc=1, device_id=plane_peer(k)[1], device_id_type=MESH)
    greetings = plane - 1 + jnp.where(above, 1, 0) + jnp.where(below, 1, 0)

    loads = []
    for i, (src, dst) in enumerate(
        ((v_hbm, v_ref), (rhs_hbm, rhs_ref), (links_hbm, links), (er_hbm, er_ref), (ei_hbm, ei_ref))
    ):
        c = pltpu.make_async_copy(src, dst, in_sem.at[i])
        c.start()
        loads.append(c)

    def neighbours(axis, index, n):
        base = {"ta": it, "gz": iz, "xy": ix}
        up, down = dict(base), dict(base)
        up[axis] = lax.rem(index + 1, n)
        down[axis] = lax.rem(index + n - 1, n)
        return up, down

    outgoing, groups, slot = [], {}, 0
    for axis, index, n, d in (("ta", it, nt, 1), ("xy", ix, nx, 3), ("gz", iz, nz, 2)):
        up, down = neighbours(axis, index, n)
        if n == 2:
            outgoing.append((axis, slot, up))
            groups[axis] = [(slot, (d, d + 4))]
            slot += 1
        else:
            turn = jnp.where(index == n - 1, 1, 0)
            for t in (turn, 1 - turn):
                target = dict(up)
                target[axis] = lax.rem(index + n - 1 + 2 * t, n)
                outgoing.append((axis, slot + t, target))
            groups[axis] = [(slot, (d,)), (slot + 1, (d + 4,))]
            slot += 2
    far, near = groups["ta"], groups["xy"] + groups["gz"]
    sends = []

    def send_to(rnd, src, y, targets, start=True):
        out = []
        for axis, s, target in targets:
            c = pltpu.make_async_remote_copy(
                src_ref=src.at[y], dst_ref=halos.at[rnd, s, y],
                send_sem=halo_send.at[rnd, s, y], recv_sem=halo_recv.at[rnd, s, y],
                device_id=target, device_id_type=MESH,
            )
            if start:
                c.start()
            out.append(c)
        sends.extend(out)
        return out

    first_far, second_far = outgoing[:1], outgoing[1 : len(far)]
    beside = outgoing[len(far) :]

    def send_far(rnd, src, y):
        send_to(rnd, src, y, first_far)
        if rnd == LAG:
            if y:
                send_to(rnd, src, y - 1, second_far)
            if y == ny - 1:
                send_to(rnd, src, y, second_far)
        else:
            send_to(rnd, src, y, second_far)

    def send_chunk(rnd, src, y):
        send_far(rnd, src, y)
        send_to(rnd, src, y, beside)

    def arrived(rnd, s, y):
        pltpu.make_async_remote_copy(
            src_ref=v_ref.at[y], dst_ref=halos.at[rnd, s, y],
            send_sem=halo_send.at[rnd, s, y], recv_sem=halo_recv.at[rnd, s, y],
            device_id=outgoing[0][2], device_id_type=MESH,
        ).wait_recv()

    def share(buf, mine, n, peer, send, recv):
        out = []
        for k in range(1, n):
            c = pltpu.make_async_remote_copy(
                src_ref=buf.at[mine], dst_ref=buf.at[mine],
                send_sem=send.at[k], recv_sem=recv.at[k],
                device_id=peer(k)[1], device_id_type=MESH,
            )
            c.start()
            out.append(c)
        sends.extend(out)
        return out

    def recv_all(copies):
        for c in copies:
            c.wait_recv()

    def add_slots(buf, n):
        parts = [buf[p] for p in range(n)]
        while len(parts) > 1:
            odd = parts[len(parts) // 2 * 2 :]
            parts = [a + b for a, b in zip(parts[::2], parts[1::2])] + odd
        return parts[0]

    lane = lax.broadcasted_iota(jnp.int32, (1, lanes), 1)
    low = lane < half
    jsign = jnp.where(low, -1.0, 1.0).astype(F32)

    def swap(x):
        return pltpu.roll(x, half, 1)

    def real(c):
        return jnp.where(low, c, swap(c))

    def imag(c):
        return jnp.where(low, swap(c), c)

    def times(f, x):
        return f[0] * x + f[1] * swap(x)

    inner = above & below

    def start_when(test, copies):
        @pl.when(test)
        def _():
            for c in copies:
                c.start()

    loads[0].wait()
    pl.semaphore_wait(barrier, greetings)
    if nt > 2:
        signal_when(it == nt - 2, token.at[0], it - 1)
        signal_when(it == 1, token.at[1], it + 1)
    wrapped = []
    for y in range(ny):
        send_to(0, v_ref, y, second_far)
        wrapped += send_to(0, v_ref, y, first_far, False)
    start_when(inner, wrapped)
    loads[1].wait()
    rows = pair(v_ref[...].reshape(ny * dof, lanes))
    cross = lax.dot_general(
        rows, pair(rhs_ref[...].reshape(ny * dof, lanes)), (((0,), (0,)), ((), ())),
        preferred_element_type=F32,
    )
    cross = cross[:lanes, :lanes] + (cross[:lanes, lanes:] + cross[lanes:, :lanes])
    corr = cross[:half] - jsign * swap(cross[half:])
    for p in range(plane):
        cpart[p] = corr[p * part : (p + 1) * part]
    rs_copies = []
    for k in range(1, plane):
        p, target = plane_peer(k)
        c = pltpu.make_async_remote_copy(
            src_ref=cpart.at[p], dst_ref=rs_buf.at[me],
            send_sem=rs_send.at[k], recv_sem=rs_recv.at[k],
            device_id=target, device_id_type=MESH,
        )
        c.start()
        rs_copies.append(c)
    rs_buf[me] = cpart[me]
    sends += rs_copies
    if nt > 2:
        wait_when(it < nt - 2, token.at[0])
        signal_when((it < nt - 2) & below, token.at[0], it - 1)
        wait_when(it > 1, token.at[1])
        signal_when((it > 1) & above, token.at[1], it + 1)
    start_when(jnp.logical_not(inner), wrapped)
    for y in range(ny):
        send_to(0, v_ref, y, beside)

    loads[3].wait()
    loads[4].wait()
    theta = half / jnp.sum(er_ref[...], axis=1, keepdims=True)
    eye = lax.broadcasted_iota(jnp.int32, (half, half), 0) == lax.broadcasted_iota(
        jnp.int32, (half, half), 1
    )
    er = jnp.sum(jnp.where(eye, er_ref[...], 0.0), axis=1, keepdims=True)
    ei = jnp.sum(jnp.where(eye, ei_ref[...], 0.0), axis=1, keepdims=True)
    scale = 1.0 / (er * er + ei * ei)
    ec[0] = er * scale + jnp.zeros((half, lanes), F32)
    ec[1] = -jsign * (ei * scale)

    loads[2].wait()
    two = 2 * dof
    valid = lane < two

    def pick(ds, b, j):
        at = j * two
        base, off = (at // 128) * 128, at % 128
        start = pl.multiple_of(b * (4 * two), 128) + base
        width = 128 if off + two <= 128 else 256
        x = [links[d, :, pl.ds(start, width)] for d in ds]
        x = jnp.concatenate(x, 0) if len(x) > 1 else x[0]
        if off:
            x = pltpu.roll(x, width - off, 1)
        return jnp.where(valid, x[:, :128], 0.0)

    def relayout(b, carry):
        for ds in ((0, 1), (2, 3), (4, 5), (6, 7), (8,)):
            for j in range(4):
                row = ds[0] * ny * dof + 4 * b + j
                flat[pl.ds(row, len(ds) * ny, stride=dof), :] = pick(ds, b, j)
        return carry

    lax.fori_loop(0, dof // 4, relayout, 0)

    def direction(y, d):
        return flat[pl.ds((d * ny + y) * dof, dof), :]

    local_group = [(0,), (4,), (8,)]
    near_group = [ds for _, ds in near]
    far_group = [ds for _, ds in far]
    widths = [pad_to(len(g) * dof, 128) for g in (local_group, near_group, far_group)]
    bases = [0, widths[0], widths[0] + widths[1]]
    first_half = lane < dof
    diag = jnp.where(
        lax.broadcasted_iota(jnp.int32, (dof, lanes), 0)
        == lax.broadcasted_iota(jnp.int32, (dof, lanes), 1), 1.0, 0.0,
    )

    def place(parts, width):
        tiles = [jnp.zeros((dof, 128), F32)] * (width // 128)
        for m, p in enumerate(parts):
            t, w = divmod(dof * m, 128)
            r = pltpu.roll(p, w, 1) if w else p
            if w + dof <= 128:
                tiles[t] = tiles[t] + r
            else:
                tiles[t] = tiles[t] + jnp.where(lane >= w, r, 0.0)
                tiles[t + 1] = tiles[t + 1] + jnp.where(lane < w, r, 0.0)
        return jnp.concatenate(tiles, 1)

    def build(y):
        for g, group in enumerate((local_group, near_group, far_group)):
            res, ims = [], []
            for ds in group:
                x = direction(y, ds[0])
                for d in ds[1:]:
                    x = x + direction(y, d)
                x = x * theta
                if not ds[0]:
                    x = diag - x
                res.append(jnp.where(first_half, x, 0.0))
                ims.append(jnp.where(first_half, pltpu.roll(x, 128 - dof, 1), 0.0))
            for h, parts in enumerate((res, ims)):
                for i, piece in enumerate(split(place(parts, widths[g]))):
                    row = (2 * i + h) * dof
                    mats[y, row : row + dof, bases[g] : bases[g] + widths[g]] = piece

    def product(y, g, blocks):
        width = widths[g]
        rest = width - len(blocks) * dof
        if rest:
            blocks = blocks + [jnp.zeros((rest, 2 * lanes), BF16)]
        out = jnp.dot(
            mats[y, :, bases[g] : bases[g] + width], jnp.concatenate(blocks, 0),
            preferred_element_type=F32,
        )
        return out[:two, :lanes] + (out[:two, lanes:] + out[two:, :lanes])

    def begin(a=0):
        for y in range(ny):
            acc[a, y] = product(y, 0, [pcs[y], pcs[(y + 1) % ny], pcs[(y - 1) % ny]])

    def halo_blocks(rnd, y, group):
        blocks = []
        for s, _ in group:
            arrived(rnd, s, y)
            blocks.append(pair(halos[rnd, s, y]))
        return blocks

    def middle(rnd, y, a=0):
        acc[a, y] += product(y, 1, halo_blocks(rnd, y, near))

    def finish(rnd, y, a=0):
        t = acc[a, y] + product(y, 2, halo_blocks(rnd, y, far))
        return t[:dof] + jsign * swap(t[dof:])

    recv_all(rs_copies)
    ct_buf[it] = add_slots(rs_buf, plane)
    ct_copies = share(ct_buf, it, nt, time_peer, ct_send, ct_recv)
    for y in range(EARLY):
        send_far(1, rhs_ref, y)
    for y in range(ny):
        send_to(1, rhs_ref, y, beside)

    for y in range(ny):
        build(y)
    for y in range(ny):
        pcs[y] = pair(v_ref[y])
    begin()

    inverse = 1.0 / theta
    for y in range(ny):
        middle(0, y)
    for y in range(ny):
        v = v_ref[y]
        w = (v - finish(0, y)) * inverse
        image_ref[y] = w
        send_far(2, image_ref, y)
        if y + EARLY < ny:
            send_far(1, rhs_ref, y + EARLY)
        for i, piece in enumerate(split(w) + split(v)):
            vw[y, i * dof : (i + 1) * dof] = piece
    recv_all(ct_copies)
    total = add_slots(ct_buf, nt)
    mine = pl.ds(me * part, part)
    ag_buf[me] = total * ec[0, mine] + swap(total) * ec[1, mine]
    ag_copies = share(ag_buf, me, plane, plane_peer, ag_send, ag_recv)
    for y in range(ny):
        send_to(2, image_ref, y, beside)
    for y in range(ny):
        pcs[y] = pair(rhs_ref[y])
    begin()
    for y in range(ny):
        middle(1, y)

    for y in range(ny):
        pcs[y] = pair(image_ref[y])
    begin(1)
    for y in range(ny):
        middle(2, y, 1)

    recv_all(ag_copies)
    coef = jnp.concatenate([ag_buf[p] for p in range(plane)], 0)
    block = pair(jnp.concatenate([coef, jsign * swap(coef)], 0))

    def expand(left):
        out = jnp.dot(left, block, preferred_element_type=F32)
        return out[:dof, :lanes] + (out[:dof, lanes:] + out[dof:, :lanes])

    for y in range(ny):
        r = finish(1, y) - expand(jnp.concatenate(split(finish(2, y, 1)), 0))
        fields[1, y] = r
        send_chunk(3, fields.at[1], y)
        pcs[y] = pair(r)
    for y in range(ny):
        fields[0, y] = rhs_ref[y] - expand(vw[y, :two])
        start_ref[y] = expand(vw[y, two:])

    def fold(x):
        return jnp.sum(x.reshape(dof // 8, 8, lanes), axis=0)

    def partials(x0, x1, x2):
        u0, u1 = x0 - x1, x1 - x2
        s0, t0 = swap(x0), swap(u0)
        return [
            fold(p)
            for p in (u0 * x0, u1 * x0, u1 * u0, u0 * u0, u0 * s0, u1 * s0, u1 * t0, u1 * u1)
        ]

    def add(a, b):
        return b if a is None else [p + q for p, q in zip(a, b)]

    def gram(sums):
        row = lax.broadcasted_iota(jnp.int32, (8, lanes), 0)
        x = jnp.sum(sums[7], axis=0, keepdims=True)
        for i in range(7):
            x = jnp.where(row == i, jnp.sum(sums[i], axis=0, keepdims=True), x)
        r = swap(x)
        y = r + jnp.where((row < 4) | (row == 7), x, -x)
        return jnp.where(low, y[:4], y[4:])

    def product_of(x, y):
        return x[0] * y[0] - x[1] * y[1], x[0] * y[1] + x[1] * y[0]

    def inner(x, y):
        return x[0] * y[0] + x[1] * y[1], x[0] * y[1] - x[1] * y[0]

    def steps(total):
        r, i = real(total), imag(total)
        a, b, c = ((r[k : k + 1], i[k : k + 1]) for k in range(3))
        size, other = r[3:4], i[3:4]
        b0 = (a[0] / size, a[1] / size)
        power = b0[0] * b0[0] + b0[1] * b0[1]
        num = inner(b0, b)
        num = (num[0] - power * c[0], num[1] - power * c[1])
        left = (1.0 - b0[0], -b0[1])
        e = product_of(left, inner(b0, c))
        den = (left[0] * left[0] + left[1] * left[1]) * size + power * other + 2.0 * e[0]
        b1 = (num[0] / den, num[1] / den)
        both = product_of(b0, b1)
        mixed = tuple(p + q - t for p, q, t in zip(b0, b1, both))
        poly = ((1.0 - mixed[0], -mixed[1]), tuple(p - q for p, q in zip(mixed, both)), both)
        poly = [(p, q * jsign) for p, q in poly]
        gain = [(theta * p, theta * q * jsign) for p, q in (mixed, both)]
        return poly, gain

    def combine(poly, xs):
        out = times(poly[0], xs[0])
        for p, x in zip(poly[1:], xs[1:]):
            out = out + times(p, x)
        return out

    def step(rnd, y):
        out = finish(rnd, y)
        fields[rnd - 1, y] = out
        if rnd < rounds - 1:
            send_chunk(rnd + 1, fields.at[rnd - 1], y)
            pcs[y] = pair(out)

    poly = gain = None
    sums = None
    rounds = SWEEPS + 2
    for rnd in range(3, rounds):
        begin()
        if rnd == 4:
            for y in range(ny):
                sums = add(sums, partials(fields[0, y], fields[1, y], fields[2, y]))
            st_buf[0, it] = gram(sums)
            early = share(st_buf.at[0], it, nt, time_peer, st_send.at[0], st_recv.at[0])
        if rnd == 5:
            recv_all(early)
            sp_buf[0, me] = add_slots(st_buf.at[0], nt)
            early = share(sp_buf.at[0], me, plane, plane_peer, sp_send.at[0], sp_recv.at[0])
        for y in range(ny + LEAD):
            if y < ny:
                middle(rnd, y)
            if y >= LEAD:
                step(rnd, y - LEAD)
    recv_all(early)
    poly, gain = steps(add_slots(sp_buf.at[0], plane))
    sums = None
    for y in range(ny):
        f = [fields[i, y] for i in range(SWEEPS + 1)]
        g = [combine(poly, f[i : i + 3]) for i in range(3)]
        for i in range(3):
            g_ref[2 * i, y] = g[i]
            g_ref[2 * i + 1, y] = swap(g[i])
        start_ref[y] = start_ref[y] + combine(gain, f[:2])
        sums = add(sums, partials(*g))
    def drain():
        for c in sends:
            c.wait_send()

    if direct:
        sd_buf[rank] = gram(sums)
        for j in range(everyone - 1):
            c = pltpu.make_async_remote_copy(
                src_ref=sd_buf.at[rank], dst_ref=sd_buf.at[rank],
                send_sem=sd_send.at[j], recv_sem=sd_recv.at[rank],
                device_id=other(j)[1], device_id_type=MESH,
            )
            c.start()
            sends.append(c)
        drain()
        for j in range(everyone - 1):
            p, target = other(j)
            pltpu.make_async_remote_copy(
                src_ref=sd_buf.at[p], dst_ref=sd_buf.at[p],
                send_sem=sd_send.at[j], recv_sem=sd_recv.at[p],
                device_id=target, device_id_type=MESH,
            ).wait_recv()
        total = add_slots(sd_buf, everyone)
    else:
        st_buf[1, it] = gram(sums)
        last = share(st_buf.at[1], it, nt, time_peer, st_send.at[1], st_recv.at[1])
        recv_all(last)
        sp_buf[1, me] = add_slots(st_buf.at[1], nt)
        last = share(sp_buf.at[1], me, plane, plane_peer, sp_send.at[1], sp_recv.at[1])
        drain()
        recv_all(last)
        total = add_slots(sp_buf.at[1], plane)
    poly, gain = steps(total)
    def blend(f, y):
        out = f[0][0] * g_ref[0, y] + f[0][1] * g_ref[1, y]
        for i in range(1, len(f)):
            out = out + (f[i][0] * g_ref[2 * i, y] + f[i][1] * g_ref[2 * i + 1, y])
        return out

    for y in range(ny):
        sol_ref[y] = start_ref[y] + blend(gain, y)
        res_ref[y] = blend(poly, y)


def hand_over(a_ref, b_ref, sol_ref, res_ref):
    sol_ref[...] = a_ref[...]
    res_ref[...] = b_ref[...]


def local(sizes, links, eigvecs, eig_real, eig_imag, rhs):
    nt, nz, nx = sizes
    plane = nz * nx
    ny, dof, lanes = rhs.shape[3:]
    half = lanes // 2
    field = (ny, dof, lanes)
    ndir = links.shape[4]
    slots = sum(1 if n == 2 else 2 for n in sizes)
    far = 1 if nt == 2 else 2
    part = half // plane
    rounds = SWEEPS + 2
    everyone = nt * plane
    direct = everyone if everyone <= DIRECT else 1
    width = sum(pad_to(n * dof, 128) for n in (3, slots - far, far))
    vmem, dma = pltpu.VMEM, pltpu.SemaphoreType.DMA
    spec = pl.BlockSpec(memory_space=pltpu.VMEM)
    sol, res = pl.pallas_call(
        functools.partial(kernel, sizes, field),
        out_shape=[vmem(field, F32)] * 2,
        in_specs=[pl.BlockSpec(memory_space=pl.ANY)] * 5,
        out_specs=[spec] * 2,
        scratch_shapes=[
            vmem((ndir, ny, links.shape[5]), F32),
            vmem(field, F32),
            vmem(field, F32),
            vmem((1, half), F32),
            vmem((1, half), F32),
            vmem((ndir * ny * dof, 128), F32),
            vmem((ny, 4 * dof, width), BF16),
            vmem((2, ny, 2 * dof, lanes), F32),
            vmem((ny, dof, 2 * lanes), BF16),
            vmem((SWEEPS + 1,) + field, F32),
            vmem((rounds, slots) + field, F32),
            vmem((ny, 4 * dof, lanes), BF16),
            vmem(field, F32),
            vmem(field, F32),
            vmem((6,) + field, F32),
            vmem((plane, part, lanes), F32),
            vmem((plane, part, lanes), F32),
            vmem((nt, part, lanes), F32),
            vmem((plane, part, lanes), F32),
            vmem((2, half, lanes), F32),
            vmem((2, nt, 4, lanes), F32),
            vmem((2, plane, 4, lanes), F32),
            vmem((direct, 4, lanes), F32),
            pltpu.SemaphoreType.REGULAR((2,)),
            dma((5,)),
            dma((rounds, slots, ny)),
            dma((rounds, slots, ny)),
            dma((plane,)),
            dma((plane,)),
            dma((nt,)),
            dma((nt,)),
            dma((plane,)),
            dma((plane,)),
            dma((2, nt)),
            dma((2, nt)),
            dma((2, plane)),
            dma((2, plane)),
            dma((direct,)),
            dma((direct,)),
        ],
        compiler_params=pltpu.CompilerParams(collective_id=0, has_side_effects=True),
    )(
        links.reshape(links.shape[3:]).transpose(1, 0, 2),
        eigvecs.reshape(field),
        eig_real.reshape(1, -1),
        eig_imag.reshape(1, -1),
        rhs.reshape(field),
    )
    sol, res = pl.pallas_call(
        hand_over,
        out_shape=[jax.ShapeDtypeStruct(field, F32)] * 2,
        in_specs=[spec] * 2,
        out_specs=[spec] * 2,
    )(*(pltpu.with_memory_space_constraint(x, pltpu.VMEM) for x in (sol, res)))
    return (sol.reshape(rhs.shape), res.reshape(rhs.shape))


def solution(mesh):
    whole = P("ta", "gz", "xy", None, None, None)
    sizes = tuple(mesh.shape[a] for a in ("ta", "gz", "xy"))
    return jax.shard_map(
        functools.partial(local, sizes),
        mesh=mesh,
        in_specs=(whole, whole, P(), P(), whole),
        out_specs=(whole, whole),
        check_vma=False,
    )
```

```python
import functools

import jax
import jax.numpy as jnp
from jax import lax
from jax.experimental import pallas as pl
from jax.experimental.pallas import tpu as pltpu
from jax.sharding import PartitionSpec as P

SWEEPS = 4
LEAD = 0
LAG = 5
EARLY = 4
DIRECT = 32
MESH = pl.DeviceIdType.MESH
F32, BF16 = jnp.float32, jnp.bfloat16


def split(x):
    first = x.astype(BF16)
    return first, (x - first.astype(F32)).astype(BF16)


def pair(x):
    return jnp.concatenate(split(x), 1)


def pad_to(n, m):
    return -(-n // m) * m


def kernel(
    sizes, dims, links_hbm, v_hbm, er_hbm, ei_hbm, rhs_hbm, sol_ref, res_ref,
    links, v_ref, rhs_ref, er_ref, ei_ref, flat, mats, acc, pcs, fields, halos, vw, image_ref, start_ref,
    g_ref, cpart, rs_buf, ct_buf, ag_buf, ec, st_buf, sp_buf, sd_buf,
    token, in_sem, halo_send, halo_recv, rs_send, rs_recv, ct_send, ct_recv, ag_send, ag_recv,
    st_send, st_recv, sp_send, sp_recv, sd_send, sd_recv,
):
    nt, nz, nx = sizes
    ny, dof, lanes = dims
    half = lanes // 2
    plane = nz * nx
    it, iz, ix = lax.axis_index("ta"), lax.axis_index("gz"), lax.axis_index("xy")
    me = iz * nx + ix
    part = half // plane

    def ranked(*ns):
        steps = [()]
        for n in ns:
            steps = [o + (d,) for o in steps for d in range(n)]
        steps.sort(key=lambda o: -sum(min(d, n - d) for d, n in zip(o, ns)))
        return steps[-1:] + steps[:-1]

    plane_steps = ranked(nz, nx)

    def plane_peer(k):
        dz, dx = plane_steps[k]
        z, x = lax.rem(iz + dz, nz), lax.rem(ix + dx, nx)
        return z * nx + x, {"ta": it, "gz": z, "xy": x}

    def time_peer(k):
        p = lax.rem(it + k, nt)
        return p, {"ta": p, "gz": iz, "xy": ix}

    everyone = nt * plane
    rank = it * plane + me

    def other(j):
        p = j + jnp.where(rank <= j, 1, 0)
        r = lax.rem(p, plane)
        return p, {"ta": lax.div(p, plane), "gz": lax.div(r, nx), "xy": lax.rem(r, nx)}

    direct = everyone <= DIRECT
    barrier = pltpu.get_barrier_semaphore()

    def at_time(p):
        return {"ta": p, "gz": iz, "xy": ix}

    def signal_when(test, sem, p):
        @pl.when(test)
        def _():
            pl.semaphore_signal(sem, inc=1, device_id=at_time(p), device_id_type=MESH)

    def wait_when(test, sem):
        @pl.when(test)
        def _():
            pl.semaphore_wait(sem, 1)

    above, below = it < nt - 1, it > 0
    signal_when(above, barrier, it + 1)
    signal_when(below, barrier, it - 1)
    for k in range(1, plane):
        pl.semaphore_signal(barrier, inc=1, device_id=plane_peer(k)[1], device_id_type=MESH)
    greetings = plane - 1 + jnp.where(above, 1, 0) + jnp.where(below, 1, 0)

    loads = []
    for i, (src, dst) in enumerate(
        ((v_hbm, v_ref), (rhs_hbm, rhs_ref), (links_hbm, links), (er_hbm, er_ref), (ei_hbm, ei_ref))
    ):
        c = pltpu.make_async_copy(src, dst, in_sem.at[i])
        c.start()
        loads.append(c)

    def neighbours(axis, index, n):
        base = {"ta": it, "gz": iz, "xy": ix}
        up, down = dict(base), dict(base)
        up[axis] = lax.rem(index + 1, n)
        down[axis] = lax.rem(index + n - 1, n)
        return up, down

    outgoing, groups, slot = [], {}, 0
    for axis, index, n, d in (("ta", it, nt, 1), ("xy", ix, nx, 3), ("gz", iz, nz, 2)):
        up, down = neighbours(axis, index, n)
        if n == 2:
            outgoing.append((axis, slot, up))
            groups[axis] = [(slot, (d, d + 4))]
            slot += 1
        else:
            turn = jnp.where(index == n - 1, 1, 0)
            for t in (turn, 1 - turn):
                target = dict(up)
                target[axis] = lax.rem(index + n - 1 + 2 * t, n)
                outgoing.append((axis, slot + t, target))
            groups[axis] = [(slot, (d,)), (slot + 1, (d + 4,))]
            slot += 2
    far, near = groups["ta"], groups["xy"] + groups["gz"]
    sends = []

    def send_to(rnd, src, y, targets, start=True):
        out = []
        for axis, s, target in targets:
            c = pltpu.make_async_remote_copy(
                src_ref=src.at[y], dst_ref=halos.at[rnd, s, y],
                send_sem=halo_send.at[rnd, s, y], recv_sem=halo_recv.at[rnd, s, y],
                device_id=target, device_id_type=MESH,
            )
            if start:
                c.start()
            out.append(c)
        sends.extend(out)
        return out

    first_far, second_far = outgoing[:1], outgoing[1 : len(far)]
    beside = outgoing[len(far) :]

    def send_far(rnd, src, y):
        send_to(rnd, src, y, first_far)
        if rnd == LAG:
            if y:
                send_to(rnd, src, y - 1, second_far)
            if y == ny - 1:
                send_to(rnd, src, y, second_far)
        else:
            send_to(rnd, src, y, second_far)

    def send_chunk(rnd, src, y):
        send_far(rnd, src, y)
        send_to(rnd, src, y, beside)

    def arrived(rnd, s, y):
        pltpu.make_async_remote_copy(
            src_ref=v_ref.at[y], dst_ref=halos.at[rnd, s, y],
            send_sem=halo_send.at[rnd, s, y], recv_sem=halo_recv.at[rnd, s, y],
            device_id=outgoing[0][2], device_id_type=MESH,
        ).wait_recv()

    def share(buf, mine, n, peer, send, recv):
        out = []
        for k in range(1, n):
            c = pltpu.make_async_remote_copy(
                src_ref=buf.at[mine], dst_ref=buf.at[mine],
                send_sem=send.at[k], recv_sem=recv.at[k],
                device_id=peer(k)[1], device_id_type=MESH,
            )
            c.start()
            out.append(c)
        sends.extend(out)
        return out

    def recv_all(copies):
        for c in copies:
            c.wait_recv()

    def add_slots(buf, n):
        parts = [buf[p] for p in range(n)]
        while len(parts) > 1:
            odd = parts[len(parts) // 2 * 2 :]
            parts = [a + b for a, b in zip(parts[::2], parts[1::2])] + odd
        return parts[0]

    lane = lax.broadcasted_iota(jnp.int32, (1, lanes), 1)
    low = lane < half
    jsign = jnp.where(low, -1.0, 1.0).astype(F32)

    def swap(x):
        return pltpu.roll(x, half, 1)

    def real(c):
        return jnp.where(low, c, swap(c))

    def imag(c):
        return jnp.where(low, swap(c), c)

    def times(f, x):
        return f[0] * x + f[1] * swap(x)

    inner = above & below

    def start_when(test, copies):
        @pl.when(test)
        def _():
            for c in copies:
                c.start()

    loads[0].wait()
    loads[1].wait()
    rows = pair(v_ref[...].reshape(ny * dof, lanes))
    cross = lax.dot_general(
        rows, pair(rhs_ref[...].reshape(ny * dof, lanes)), (((0,), (0,)), ((), ())),
        preferred_element_type=F32,
    )
    cross = cross[:lanes, :lanes] + (cross[:lanes, lanes:] + cross[lanes:, :lanes])
    corr = cross[:half] - jsign * swap(cross[half:])
    for p in range(plane):
        cpart[p] = corr[p * part : (p + 1) * part]
    pl.semaphore_wait(barrier, greetings)
    if nt > 2:
        signal_when(it == nt - 2, token.at[0], it - 1)
        signal_when(it == 1, token.at[1], it + 1)
    wrapped = []
    for y in range(ny):
        send_to(0, v_ref, y, second_far)
        wrapped += send_to(0, v_ref, y, first_far, False)
    start_when(inner, wrapped)
    rs_copies = []
    for k in range(1, plane):
        p, target = plane_peer(k)
        c = pltpu.make_async_remote_copy(
            src_ref=cpart.at[p], dst_ref=rs_buf.at[me],
            send_sem=rs_send.at[k], recv_sem=rs_recv.at[k],
            device_id=target, device_id_type=MESH,
        )
        c.start()
        rs_copies.append(c)
    rs_buf[me] = cpart[me]
    sends += rs_copies
    if nt > 2:
        wait_when(it < nt - 2, token.at[0])
        signal_when((it < nt - 2) & below, token.at[0], it - 1)
        wait_when(it > 1, token.at[1])
        signal_when((it > 1) & above, token.at[1], it + 1)
    start_when(jnp.logical_not(inner), wrapped)
    for y in range(ny):
        send_to(0, v_ref, y, beside)

    loads[3].wait()
    loads[4].wait()
    theta = half / jnp.sum(er_ref[...], axis=1, keepdims=True)
    eye = lax.broadcasted_iota(jnp.int32, (half, half), 0) == lax.broadcasted_iota(
        jnp.int32, (half, half), 1
    )
    er = jnp.sum(jnp.where(eye, er_ref[...], 0.0), axis=1, keepdims=True)
    ei = jnp.sum(jnp.where(eye, ei_ref[...], 0.0), axis=1, keepdims=True)
    scale = 1.0 / (er * er + ei * ei)
    ec[0] = er * scale + jnp.zeros((half, lanes), F32)
    ec[1] = -jsign * (ei * scale)

    loads[2].wait()
    two = 2 * dof
    valid = lane < two

    def pick(ds, b, j):
        at = j * two
        base, off = (at // 128) * 128, at % 128
        start = pl.multiple_of(b * (4 * two), 128) + base
        width = 128 if off + two <= 128 else 256
        x = [links[d, :, pl.ds(start, width)] for d in ds]
        x = jnp.concatenate(x, 0) if len(x) > 1 else x[0]
        if off:
            x = pltpu.roll(x, width - off, 1)
        return jnp.where(valid, x[:, :128], 0.0)

    def relayout(b, carry):
        for ds in ((0, 1), (2, 3), (4, 5), (6, 7), (8,)):
            for j in range(4):
                row = ds[0] * ny * dof + 4 * b + j
                flat[pl.ds(row, len(ds) * ny, stride=dof), :] = pick(ds, b, j)
        return carry

    lax.fori_loop(0, dof // 4, relayout, 0)

    def direction(y, d):
        return flat[pl.ds((d * ny + y) * dof, dof), :]

    local_group = [(0,), (4,), (8,)]
    near_group = [ds for _, ds in near]
    far_group = [ds for _, ds in far]
    widths = [pad_to(len(g) * dof, 128) for g in (local_group, near_group, far_group)]
    bases = [0, widths[0], widths[0] + widths[1]]
    first_half = lane < dof
    diag = jnp.where(
        lax.broadcasted_iota(jnp.int32, (dof, lanes), 0)
        == lax.broadcasted_iota(jnp.int32, (dof, lanes), 1), 1.0, 0.0,
    )

    def place(parts, width):
        tiles = [jnp.zeros((dof, 128), F32)] * (width // 128)
        for m, p in enumerate(parts):
            t, w = divmod(dof * m, 128)
            r = pltpu.roll(p, w, 1) if w else p
            if w + dof <= 128:
                tiles[t] = tiles[t] + r
            else:
                tiles[t] = tiles[t] + jnp.where(lane >= w, r, 0.0)
                tiles[t + 1] = tiles[t + 1] + jnp.where(lane < w, r, 0.0)
        return jnp.concatenate(tiles, 1)

    def build(y):
        for g, group in enumerate((local_group, near_group, far_group)):
            res, ims = [], []
            for ds in group:
                x = direction(y, ds[0])
                for d in ds[1:]:
                    x = x + direction(y, d)
                x = x * theta
                if not ds[0]:
                    x = diag - x
                res.append(jnp.where(first_half, x, 0.0))
                ims.append(jnp.where(first_half, pltpu.roll(x, 128 - dof, 1), 0.0))
            for h, parts in enumerate((res, ims)):
                for i, piece in enumerate(split(place(parts, widths[g]))):
                    row = (2 * i + h) * dof
                    mats[y, row : row + dof, bases[g] : bases[g] + widths[g]] = piece

    def product(y, g, blocks):
        width = widths[g]
        rest = width - len(blocks) * dof
        if rest:
            blocks = blocks + [jnp.zeros((rest, 2 * lanes), BF16)]
        out = jnp.dot(
            mats[y, :, bases[g] : bases[g] + width], jnp.concatenate(blocks, 0),
            preferred_element_type=F32,
        )
        return out[:two, :lanes] + (out[:two, lanes:] + out[two:, :lanes])

    def begin(a=0):
        for y in range(ny):
            acc[a, y] = product(y, 0, [pcs[y], pcs[(y + 1) % ny], pcs[(y - 1) % ny]])

    def halo_blocks(rnd, y, group):
        blocks = []
        for s, _ in group:
            arrived(rnd, s, y)
            blocks.append(pair(halos[rnd, s, y]))
        return blocks

    def middle(rnd, y, a=0):
        acc[a, y] += product(y, 1, halo_blocks(rnd, y, near))

    def finish(rnd, y, a=0):
        t = acc[a, y] + product(y, 2, halo_blocks(rnd, y, far))
        return t[:dof] + jsign * swap(t[dof:])

    recv_all(rs_copies)
    ct_buf[it] = add_slots(rs_buf, plane)
    ct_copies = share(ct_buf, it, nt, time_peer, ct_send, ct_recv)
    for y in range(EARLY):
        send_far(1, rhs_ref, y)
    for y in range(ny):
        send_to(1, rhs_ref, y, beside)

    for y in range(ny):
        build(y)
    for y in range(ny):
        pcs[y] = pair(v_ref[y])
    begin()

    inverse = 1.0 / theta
    for y in range(ny):
        middle(0, y)
    for y in range(ny):
        v = v_ref[y]
        w = (v - finish(0, y)) * inverse
        image_ref[y] = w
        send_far(2, image_ref, y)
        if y + EARLY < ny:
            send_far(1, rhs_ref, y + EARLY)
        for i, piece in enumerate(split(w) + split(v)):
            vw[y, i * dof : (i + 1) * dof] = piece
    recv_all(ct_copies)
    total = add_slots(ct_buf, nt)
    mine = pl.ds(me * part, part)
    ag_buf[me] = total * ec[0, mine] + swap(total) * ec[1, mine]
    ag_copies = share(ag_buf, me, plane, plane_peer, ag_send, ag_recv)
    for y in range(ny):
        send_to(2, image_ref, y, beside)
    for y in range(ny):
        pcs[y] = pair(rhs_ref[y])
    begin()
    for y in range(ny):
        middle(1, y)

    for y in range(ny):
        pcs[y] = pair(image_ref[y])
    begin(1)
    for y in range(ny):
        middle(2, y, 1)

    recv_all(ag_copies)
    coef = jnp.concatenate([ag_buf[p] for p in range(plane)], 0)
    block = pair(jnp.concatenate([coef, jsign * swap(coef)], 0))

    def expand(left):
        out = jnp.dot(left, block, preferred_element_type=F32)
        return out[:dof, :lanes] + (out[:dof, lanes:] + out[dof:, :lanes])

    for y in range(ny):
        r = finish(1, y) - expand(jnp.concatenate(split(finish(2, y, 1)), 0))
        fields[1, y] = r
        send_chunk(3, fields.at[1], y)
        pcs[y] = pair(r)
    for y in range(ny):
        fields[0, y] = rhs_ref[y] - expand(vw[y, :two])
        start_ref[y] = expand(vw[y, two:])

    def fold(x):
        return jnp.sum(x.reshape(dof // 8, 8, lanes), axis=0)

    def partials(x0, x1, x2):
        u0, u1 = x0 - x1, x1 - x2
        s0, t0 = swap(x0), swap(u0)
        return [
            fold(p)
            for p in (u0 * x0, u1 * x0, u1 * u0, u0 * u0, u0 * s0, u1 * s0, u1 * t0, u1 * u1)
        ]

    def add(a, b):
        return b if a is None else [p + q for p, q in zip(a, b)]

    def gram(sums):
        row = lax.broadcasted_iota(jnp.int32, (8, lanes), 0)
        x = jnp.sum(sums[7], axis=0, keepdims=True)
        for i in range(7):
            x = jnp.where(row == i, jnp.sum(sums[i], axis=0, keepdims=True), x)
        r = swap(x)
        y = r + jnp.where((row < 4) | (row == 7), x, -x)
        return jnp.where(low, y[:4], y[4:])

    def product_of(x, y):
        return x[0] * y[0] - x[1] * y[1], x[0] * y[1] + x[1] * y[0]

    def inner(x, y):
        return x[0] * y[0] + x[1] * y[1], x[0] * y[1] - x[1] * y[0]

    def steps(total):
        r, i = real(total), imag(total)
        a, b, c = ((r[k : k + 1], i[k : k + 1]) for k in range(3))
        size, other = r[3:4], i[3:4]
        b0 = (a[0] / size, a[1] / size)
        power = b0[0] * b0[0] + b0[1] * b0[1]
        num = inner(b0, b)
        num = (num[0] - power * c[0], num[1] - power * c[1])
        left = (1.0 - b0[0], -b0[1])
        e = product_of(left, inner(b0, c))
        den = (left[0] * left[0] + left[1] * left[1]) * size + power * other + 2.0 * e[0]
        b1 = (num[0] / den, num[1] / den)
        both = product_of(b0, b1)
        mixed = tuple(p + q - t for p, q, t in zip(b0, b1, both))
        poly = ((1.0 - mixed[0], -mixed[1]), tuple(p - q for p, q in zip(mixed, both)), both)
        poly = [(p, q * jsign) for p, q in poly]
        gain = [(theta * p, theta * q * jsign) for p, q in (mixed, both)]
        return poly, gain

    def combine(poly, xs):
        out = times(poly[0], xs[0])
        for p, x in zip(poly[1:], xs[1:]):
            out = out + times(p, x)
        return out

    def step(rnd, y):
        out = finish(rnd, y)
        fields[rnd - 1, y] = out
        if rnd < rounds - 1:
            send_chunk(rnd + 1, fields.at[rnd - 1], y)
            pcs[y] = pair(out)

    poly = gain = None
    sums = None
    rounds = SWEEPS + 2
    for rnd in range(3, rounds):
        begin()
        if rnd == 4:
            for y in range(ny):
                sums = add(sums, partials(fields[0, y], fields[1, y], fields[2, y]))
            st_buf[0, it] = gram(sums)
            early = share(st_buf.at[0], it, nt, time_peer, st_send.at[0], st_recv.at[0])
        if rnd == 5:
            recv_all(early)
            sp_buf[0, me] = add_slots(st_buf.at[0], nt)
            early = share(sp_buf.at[0], me, plane, plane_peer, sp_send.at[0], sp_recv.at[0])
        for y in range(ny + LEAD):
            if y < ny:
                middle(rnd, y)
            if y >= LEAD:
                step(rnd, y - LEAD)
    recv_all(early)
    poly, gain = steps(add_slots(sp_buf.at[0], plane))
    sums = None
    for y in range(ny):
        f = [fields[i, y] for i in range(SWEEPS + 1)]
        g = [combine(poly, f[i : i + 3]) for i in range(3)]
        for i in range(3):
            g_ref[2 * i, y] = g[i]
            g_ref[2 * i + 1, y] = swap(g[i])
        start_ref[y] = start_ref[y] + combine(gain, f[:2])
        sums = add(sums, partials(*g))
    def drain():
        for c in sends:
            c.wait_send()

    if direct:
        sd_buf[rank] = gram(sums)
        for j in range(everyone - 1):
            c = pltpu.make_async_remote_copy(
                src_ref=sd_buf.at[rank], dst_ref=sd_buf.at[rank],
                send_sem=sd_send.at[j], recv_sem=sd_recv.at[rank],
                device_id=other(j)[1], device_id_type=MESH,
            )
            c.start()
            sends.append(c)
        drain()
        for j in range(everyone - 1):
            p, target = other(j)
            pltpu.make_async_remote_copy(
                src_ref=sd_buf.at[p], dst_ref=sd_buf.at[p],
                send_sem=sd_send.at[j], recv_sem=sd_recv.at[p],
                device_id=target, device_id_type=MESH,
            ).wait_recv()
        total = add_slots(sd_buf, everyone)
    else:
        st_buf[1, it] = gram(sums)
        last = share(st_buf.at[1], it, nt, time_peer, st_send.at[1], st_recv.at[1])
        recv_all(last)
        sp_buf[1, me] = add_slots(st_buf.at[1], nt)
        last = share(sp_buf.at[1], me, plane, plane_peer, sp_send.at[1], sp_recv.at[1])
        drain()
        recv_all(last)
        total = add_slots(sp_buf.at[1], plane)
    poly, gain = steps(total)
    def blend(f, y):
        out = f[0][0] * g_ref[0, y] + f[0][1] * g_ref[1, y]
        for i in range(1, len(f)):
            out = out + (f[i][0] * g_ref[2 * i, y] + f[i][1] * g_ref[2 * i + 1, y])
        return out

    for y in range(ny):
        sol_ref[y] = start_ref[y] + blend(gain, y)
        res_ref[y] = blend(poly, y)


def hand_over(a_ref, b_ref, sol_ref, res_ref):
    sol_ref[...] = a_ref[...]
    res_ref[...] = b_ref[...]


def local(sizes, links, eigvecs, eig_real, eig_imag, rhs):
    nt, nz, nx = sizes
    plane = nz * nx
    ny, dof, lanes = rhs.shape[3:]
    half = lanes // 2
    field = (ny, dof, lanes)
    ndir = links.shape[4]
    slots = sum(1 if n == 2 else 2 for n in sizes)
    far = 1 if nt == 2 else 2
    part = half // plane
    rounds = SWEEPS + 2
    everyone = nt * plane
    direct = everyone if everyone <= DIRECT else 1
    width = sum(pad_to(n * dof, 128) for n in (3, slots - far, far))
    vmem, dma = pltpu.VMEM, pltpu.SemaphoreType.DMA
    spec = pl.BlockSpec(memory_space=pltpu.VMEM)
    sol, res = pl.pallas_call(
        functools.partial(kernel, sizes, field),
        out_shape=[vmem(field, F32)] * 2,
        in_specs=[pl.BlockSpec(memory_space=pl.ANY)] * 5,
        out_specs=[spec] * 2,
        scratch_shapes=[
            vmem((ndir, ny, links.shape[5]), F32),
            vmem(field, F32),
            vmem(field, F32),
            vmem((1, half), F32),
            vmem((1, half), F32),
            vmem((ndir * ny * dof, 128), F32),
            vmem((ny, 4 * dof, width), BF16),
            vmem((2, ny, 2 * dof, lanes), F32),
            vmem((ny, dof, 2 * lanes), BF16),
            vmem((SWEEPS + 1,) + field, F32),
            vmem((rounds, slots) + field, F32),
            vmem((ny, 4 * dof, lanes), BF16),
            vmem(field, F32),
            vmem(field, F32),
            vmem((6,) + field, F32),
            vmem((plane, part, lanes), F32),
            vmem((plane, part, lanes), F32),
            vmem((nt, part, lanes), F32),
            vmem((plane, part, lanes), F32),
            vmem((2, half, lanes), F32),
            vmem((2, nt, 4, lanes), F32),
            vmem((2, plane, 4, lanes), F32),
            vmem((direct, 4, lanes), F32),
            pltpu.SemaphoreType.REGULAR((2,)),
            dma((5,)),
            dma((rounds, slots, ny)),
            dma((rounds, slots, ny)),
            dma((plane,)),
            dma((plane,)),
            dma((nt,)),
            dma((nt,)),
            dma((plane,)),
            dma((plane,)),
            dma((2, nt)),
            dma((2, nt)),
            dma((2, plane)),
            dma((2, plane)),
            dma((direct,)),
            dma((direct,)),
        ],
        compiler_params=pltpu.CompilerParams(collective_id=0, has_side_effects=True),
    )(
        links.reshape(links.shape[3:]).transpose(1, 0, 2),
        eigvecs.reshape(field),
        eig_real.reshape(1, -1),
        eig_imag.reshape(1, -1),
        rhs.reshape(field),
    )
    sol, res = pl.pallas_call(
        hand_over,
        out_shape=[jax.ShapeDtypeStruct(field, F32)] * 2,
        in_specs=[spec] * 2,
        out_specs=[spec] * 2,
    )(*(pltpu.with_memory_space_constraint(x, pltpu.VMEM) for x in (sol, res)))
    return (sol.reshape(rhs.shape), res.reshape(rhs.shape))


def solution(mesh):
    whole = P("ta", "gz", "xy", None, None, None)
    sizes = tuple(mesh.shape[a] for a in ("ta", "gz", "xy"))
    return jax.shard_map(
        functools.partial(local, sizes),
        mesh=mesh,
        in_specs=(whole, whole, P(), P(), whole),
        out_specs=(whole, whole),
        check_vma=False,
    )
```
